128 devices in a mesh: sys: 1, aux: 16 (over z, y), orb: 8 (over x, core).
Axes of the slice: x: 4, y: 4, z: 4, core: 2. Of those that a mesh axis runs over, the one named last changes fastest.
Arguments:
- aux_ints: float32 [1856, 384, 384], P(('sys', 'aux'), 'orb')
- metric: float32 [1856, 1856], P(('sys', 'aux'))
- orbitals: float32 [4, 384, 80], P('sys')
Outputs:
- output: float32 [4, 384, 384], P('sys', 'orb', 'aux')
All inputs are finite; a program needn't handle non-finite values.
Results may differ from the reference program's by a relative error of at most 0.001.
Values are sent between devices in bfloat16 or wider.
A program may use at most 1 GiB of HBM per device.

```python
import jax
import jax.numpy as jnp
from jax import lax

N_AUX = 1856
N_BASIS = 384
N_OCC = 80
DENS = 4

PRECISE = lax.Precision.HIGHEST


def setup_inputs(seed: int = 0, part: int = 0) -> dict:
    base_key = jax.random.fold_in(jax.random.key(seed), part)
    sub_keys = jax.random.split(base_key, 6)
    rank_b = 4
    rank_m = 4
    coh_scale = (2.0 * N_AUX * N_OCC) ** -0.5 * rank_b ** -0.25
    noise_scale = 2.0 * coh_scale
    coeffs = jax.random.normal(sub_keys[0], (N_AUX, rank_b), jnp.float32)
    patterns = jax.random.normal(sub_keys[1], (rank_b, N_BASIS), jnp.float32)
    row_keys = jax.random.split(sub_keys[2], N_AUX)

    def one_row(row_args):
        row_key, coeff_row = row_args
        noise_mat = jax.random.normal(row_key, (N_BASIS, N_BASIS), jnp.float32)
        sym_noise = (noise_mat + noise_mat.T) * (0.5 ** 0.5)
        low_rank = jnp.einsum('k,km,kl->ml', coeff_row, patterns, patterns)
        return noise_scale * sym_noise + coh_scale * low_rank

    aux_ints = lax.map(one_row, (row_keys, coeffs))
    spread = jax.random.normal(sub_keys[3], (N_AUX, N_AUX), jnp.float32)
    sym_spread = (spread + spread.T) * (0.125 / N_AUX) ** 0.5
    directions = jax.random.normal(sub_keys[4], (rank_m, N_AUX), jnp.float32) * N_AUX ** -0.5
    boost_scale = (N_AUX / rank_m) ** 0.5
    metric = jnp.eye(N_AUX, dtype=jnp.float32) + sym_spread + boost_scale * jnp.dot(directions.T, directions)
    orbitals = jax.random.normal(sub_keys[5], (DENS, N_BASIS, N_OCC), jnp.float32) * N_BASIS ** -0.5
    return {'aux_ints': aux_ints, 'metric': metric, 'orbitals': orbitals}


def reference(aux_ints, metric, orbitals):
    def one_density(coeff_mat):
        half_tr = jnp.einsum('qml,li->qmi', aux_ints, coeff_mat, precision=PRECISE)
        fitted = jnp.einsum('pq,qmi->pmi', metric, half_tr, precision=PRECISE)
        exchange = jnp.einsum('pmi,pni->mn', fitted, fitted, precision=PRECISE)
        gamma_raw = jnp.einsum('qmi,mi->q', half_tr, coeff_mat, precision=PRECISE)
        gamma_fit = jnp.dot(metric, gamma_raw, precision=PRECISE)
        weights = jnp.dot(gamma_fit, metric, precision=PRECISE)
        coulomb = jnp.einsum('q,qmn->mn', weights, aux_ints, precision=PRECISE)
        return 2.0 * coulomb - exchange

    return lax.map(one_density, orbitals)
```

```python
import jax
import jax.numpy as jnp
from jax import lax
from jax.sharding import PartitionSpec as P

PRECISE = lax.Precision.HIGHEST
F32 = jnp.float32
BF16 = jnp.bfloat16


def solution(mesh):
    n_aux, n_orb = mesh.shape['aux'], mesh.shape['orb']
    chips = n_aux * n_orb // 2

    def local_fock(ints_blk, metric_blk, orbitals):
        q_loc, m_loc, n_bas = ints_blk.shape
        dens, _, n_occ = orbitals.shape
        cols = dens * n_occ // chips
        orb = lax.axis_index('orb')
        half = lax.rem(orb, 2)
        row_start = orb * m_loc
        p_half = q_loc // 2
        met_part = lax.dynamic_slice_in_dim(metric_blk, half * p_half, p_half, axis=0).astype(BF16)
        met = lax.all_gather(met_part, 'aux', axis=0, tiled=True)

        flat_orb = orbitals.transpose(1, 0, 2).reshape(n_bas, dens * n_occ)
        half_tr = jnp.einsum('qml,lc->cmq', ints_blk, flat_orb, precision=PRECISE, preferred_element_type=F32)

        send = half_tr.astype(BF16).reshape(chips, cols, 2, m_loc // 2, q_loc)
        send = send.transpose(0, 2, 1, 3, 4).reshape(2 * chips, cols, m_loc // 2, q_loc)
        recv = lax.all_to_all(send, ('aux', 'orb'), 0, 0, tiled=True)
        pair = [(i, i ^ 1) for i in range(n_orb)]
        other = lax.ppermute(recv, 'orb', pair)
        both = jnp.stack([jnp.where(half == 0, recv, other), jnp.where(half == 0, other, recv)])
        both = both.reshape(2, n_aux, n_orb, cols, m_loc // 2, q_loc)
        t0 = both.transpose(1, 5, 3, 2, 0, 4).reshape(n_aux * q_loc, cols * n_bas)

        orb_rows = lax.dynamic_slice_in_dim(flat_orb, row_start, m_loc, axis=0)
        gamma_part = (half_tr * orb_rows.T[:, :, None]).reshape(dens, n_occ * m_loc, q_loc).sum(1)
        gamma_raw = lax.psum(gamma_part, 'orb')
        gamma_all = lax.all_gather(gamma_raw, 'aux', axis=1, tiled=True)
        gamma_fit = jnp.einsum('dq,pq->dp', gamma_all, metric_blk, precision=PRECISE, preferred_element_type=F32)
        weight_part = jnp.dot(gamma_fit, metric_blk, precision=PRECISE, preferred_element_type=F32)
        weights = lax.psum_scatter(weight_part, 'aux', scatter_dimension=1, tiled=True)
        coulomb = jnp.einsum('dq,qmn->dmn', weights, ints_blk, precision=PRECISE, preferred_element_type=F32)
        coul = lax.psum_scatter(coulomb, 'aux', scatter_dimension=2, tiled=True)

        fitted = lax.dot(met, t0, preferred_element_type=F32)
        fitted = fitted.reshape(-1, cols, n_bas)
        part = jnp.einsum('pcm,pcn->mn', fitted, fitted, precision=PRECISE, preferred_element_type=F32)
        n_out = n_bas // n_aux
        part = part.reshape(n_orb, m_loc, n_aux, n_out).transpose(2, 0, 1, 3).reshape(n_aux * n_orb, m_loc, n_out)
        got = lax.all_to_all(part, ('aux', 'orb'), 0, 0, tiled=True)
        exch = got.reshape(dens, -1, m_loc, n_out).sum(1)
        return 2.0 * coul - exch

    return jax.shard_map(local_fock, mesh=mesh, in_specs=(P(('sys', 'aux'), 'orb', None), P(('sys', 'aux'), None), P('sys', None, None)), out_specs=P('sys', 'orb', 'aux'), check_vma=False)
```

```python
import functools

import jax
import jax.numpy as jnp
from jax import lax
from jax.experimental import pallas as pl
from jax.experimental.pallas import tpu as pltpu
from jax.sharding import PartitionSpec as P

PRECISE = lax.Precision.HIGHEST
F32 = jnp.float32
BF16 = jnp.bfloat16
LANES = 128
NT = (((1,), (1,)), ((), ()))


def split3(x):
    hi = x.astype(BF16)
    rest = x - hi.astype(F32)
    mid = rest.astype(BF16)
    lo = (rest - mid.astype(F32)).astype(BF16)
    return hi, mid, lo


def split3_xla(x):
    hi = lax.reduce_precision(x, 8, 7)
    rest = x - hi
    mid = lax.reduce_precision(rest, 8, 7)
    return hi.astype(BF16), mid.astype(BF16), (rest - mid).astype(BF16)


def left_terms(x):
    hi, mid, lo = split3_xla(x)
    return jnp.concatenate([hi, hi, mid, hi, mid, lo], axis=-1)


def half_kernel(ints_hbm, orb_ref, dens_ref, out_ref, gam_ref, ints, wide, sems):
    q_loc, m_loc, n_bas = ints_hbm.shape
    n_col = orb_ref.shape[0]
    groups = m_loc // 8
    tiles = n_bas // LANES
    copies = [
        [pltpu.make_async_copy(
            ints_hbm.at[:, pl.ds(8 * g, 8), pl.ds(LANES * t, LANES)],
            ints.at[t, pl.ds(0, q_loc), pl.ds(8 * g, 8), :], sems.at[g, t]) for t in range(tiles)]
        for g in range(groups)]
    for group in copies:
        for copy in group:
            copy.start()
    ints[:, pl.ds(q_loc, LANES - q_loc)] = jnp.zeros((tiles, LANES - q_loc, m_loc, LANES), F32)
    flat = ints.reshape(tiles, LANES * m_loc, LANES)
    gam_ref[...] = jnp.zeros_like(gam_ref)

    for g in range(groups):
        for copy in copies[g]:
            copy.wait()

        def pair_step(j, carry, g=g):
            m = 8 * g + 2 * j
            rows = jnp.concatenate([
                jnp.concatenate([flat[t, pl.ds(m + u, LANES, stride=m_loc), :] for t in range(tiles)], axis=1)
                for u in range(2)], axis=0)
            hi, mid, lo = split3(rows)
            right = jnp.concatenate([hi, mid, hi, lo, mid, hi], axis=1)
            left = jnp.concatenate([orb_ref[...], dens_ref[4 * g + j]], axis=0)
            res = lax.dot_general(left, right, NT, preferred_element_type=F32)
            wide[pl.ds(m, n_col, stride=m_loc), :] = res[:n_col, :LANES]
            wide[pl.ds(m + 1, n_col, stride=m_loc), :] = res[:n_col, LANES:]
            gam_ref[...] += res[n_col:n_col + 8, :LANES] + res[n_col + 8:, LANES:]
            return carry

        lax.fori_loop(0, 4, pair_step, 0)

    def narrow(c, carry):
        rows = m_loc * 4
        out_ref[pl.ds(pl.multiple_of(c * rows, rows), rows), :] = wide[pl.ds(pl.multiple_of(c * rows, rows), rows), :].astype(BF16)
        return carry

    lax.fori_loop(0, n_col // 4, narrow, 0)


def half_transform(ints_blk, orb_terms, dens_terms):
    q_loc, m_loc, n_bas = ints_blk.shape
    n_col, depth = orb_terms.shape
    vmem = pl.BlockSpec(memory_space=pltpu.VMEM)
    return pl.pallas_call(
        half_kernel,
        out_shape=(jax.ShapeDtypeStruct((n_col * m_loc, LANES), BF16), jax.ShapeDtypeStruct((8, LANES), F32)),
        in_specs=[pl.BlockSpec(memory_space=pl.ANY), vmem, vmem],
        out_specs=(vmem, vmem),
        scratch_shapes=[
            pltpu.VMEM((n_bas // LANES, LANES, m_loc, LANES), F32),
            pltpu.VMEM((n_col * m_loc, LANES), F32),
            pltpu.SemaphoreType.DMA((m_loc // 8, n_bas // LANES)),
        ],
        compiler_params=pltpu.CompilerParams(vmem_limit_bytes=56 * 1024 * 1024),
        cost_estimate=pl.CostEstimate(flops=2 * 6 * n_col * n_bas * q_loc * m_loc, bytes_accessed=14 << 20, transcendentals=0),
        name='half_transform',
    )(ints_blk, orb_terms, dens_terms)


def fock_kernel(half_ref, own_ref, other_ref, met_ref, out_ref, fit):
    n_src, cols, m_loc, _ = own_ref.shape
    n_aux = met_ref.shape[0]
    n_x = n_src // n_aux
    rows = n_x * m_loc
    n_fit = met_ref.shape[2]
    here = pl.multiple_of(half_ref[0] * rows, rows)
    there = pl.multiple_of((1 - half_ref[0]) * rows, rows)
    tile = 256

    def col_step(c, acc):
        for src, start in ((own_ref, here), (other_ref, there)):
            for n in range(n_fit // tile):
                tot = None
                for s in range(n_aux // 2):
                    left = jnp.concatenate([src[pl.ds((2 * s + t) * n_x, n_x), c].reshape(rows, LANES) for t in range(2)], axis=1)
                    right = met_ref[pl.ds(2 * s, 2), :, pl.ds(n * tile, tile)].reshape(2 * LANES, tile)
                    part = jnp.dot(left, right, preferred_element_type=F32)
                    tot = part if tot is None else tot + part
                fit[pl.ds(start, rows), pl.ds(n * tile, tile)] = tot
        for n in range(n_fit // tile):
            hi, mid, lo = split3(fit[:, pl.ds(n * tile, tile)])
            same = lax.dot_general(hi, hi, NT, preferred_element_type=F32) + lax.dot_general(mid, mid, NT, preferred_element_type=F32)
            cross = lax.dot_general(hi, mid, NT, preferred_element_type=F32) + lax.dot_general(hi, lo, NT, preferred_element_type=F32)
            out_ref[0] += same
            out_ref[1] += cross
        return acc

    out_ref[...] = jnp.zeros_like(out_ref)
    lax.fori_loop(0, cols, col_step, 0)
    out_ref[0] += out_ref[1] + out_ref[1].T


def exchange_part(half, own, other, met):
    n_src, cols, m_loc, _ = own.shape
    n_aux, _, n_fit = met.shape
    n_bas = 2 * m_loc * n_src // n_aux
    vmem = pl.BlockSpec(memory_space=pltpu.VMEM)
    return pl.pallas_call(
        fock_kernel,
        out_shape=jax.ShapeDtypeStruct((2, n_bas, n_bas), F32),
        in_specs=[pl.BlockSpec(memory_space=pltpu.SMEM), vmem, vmem, vmem],
        out_specs=vmem,
        scratch_shapes=[pltpu.VMEM((n_bas, n_fit), F32)],
        compiler_params=pltpu.CompilerParams(vmem_limit_bytes=56 * 1024 * 1024),
        cost_estimate=pl.CostEstimate(flops=32 << 30, bytes_accessed=14 << 20, transcendentals=0),
        name='exchange_part',
    )(half, own, other, met)


def coulomb_kernel(wt_ref, ints_ref, out_ref):
    dens, q_loc = wt_ref.shape

    def q_step(q, acc):
        row = ints_ref[q]
        return tuple(acc[d] + wt_ref[d, q] * row for d in range(dens))

    acc = lax.fori_loop(0, q_loc, q_step, tuple(jnp.zeros(ints_ref.shape[1:], F32) for _ in range(dens)), unroll=4)
    for d in range(dens):
        out_ref[d] = acc[d]


def coulomb_part(weights, ints_blk):
    q_loc, m_loc, n_bas = ints_blk.shape
    dens = weights.shape[0]
    return pl.pallas_call(
        coulomb_kernel,
        grid=(m_loc // 8,),
        out_shape=jax.ShapeDtypeStruct((dens, m_loc, n_bas), F32),
        in_specs=[pl.BlockSpec(memory_space=pltpu.SMEM), pl.BlockSpec((q_loc, 8, n_bas), lambda g: (0, g, 0))],
        out_specs=pl.BlockSpec((dens, 8, n_bas), lambda g: (0, g, 0)),
        cost_estimate=pl.CostEstimate(flops=2 * dens * q_loc * m_loc * n_bas, bytes_accessed=9 << 20, transcendentals=0),
        name='coulomb_part',
    )(weights, ints_blk)


def solution(mesh):
    n_aux, n_orb = mesh.shape['aux'], mesh.shape['orb']
    n_x = n_orb // 2
    chips = n_aux * n_x
    mesh4 = jax.sharding.Mesh(mesh.devices.reshape(1, n_aux, n_x, 2), ('sys', 'aux', 'x', 'core'))

    def local_fock(ints_blk, metric_blk, orbitals):
        q_loc, m_loc, n_bas = ints_blk.shape
        dens, _, n_occ = orbitals.shape
        cols = dens * n_occ // chips
        half = lax.axis_index('core')
        orb = lax.axis_index('x') * 2 + half
        n_fit = n_bas * 0 + 1024
        met_pad = jnp.pad(metric_blk, ((0, LANES - q_loc), (0, 2 * n_fit - metric_blk.shape[1])))
        met_part = lax.dynamic_slice_in_dim(met_pad, half * n_fit, n_fit, axis=1).astype(BF16)
        met = lax.all_gather(met_part, 'aux', axis=0)

        orb_rows = lax.dynamic_slice_in_dim(orbitals, orb * m_loc, m_loc, axis=1)
        dens_rows = jnp.einsum('dmi,dli->mdl', orb_rows, orbitals, precision=PRECISE, preferred_element_type=F32)
        dens_rows = jnp.pad(dens_rows, ((0, 0), (0, 8 - dens), (0, 0))).reshape(m_loc // 2, 16, n_bas)
        orb_cols = orbitals.transpose(0, 2, 1).reshape(dens * n_occ, n_bas)
        half_tr, gamma = half_transform(ints_blk, left_terms(orb_cols), left_terms(dens_rows))

        gamma = jnp.broadcast_to(gamma[:dens][None], (2 * chips, dens, LANES))
        gamma_all = lax.all_to_all(gamma, ('aux', 'x', 'core'), 0, 0, tiled=True)
        own = lax.all_to_all(half_tr.reshape(chips, cols, m_loc, LANES), ('aux', 'x'), 0, 0, tiled=True)
        other = lax.ppermute(own, 'core', [(0, 1), (1, 0)])

        gamma_raw = gamma_all.reshape(n_aux, n_orb, dens, LANES).sum(1)[:, :, :q_loc].transpose(1, 0, 2).reshape(dens, n_aux * q_loc)
        gamma_fit = jnp.einsum('dq,pq->dp', gamma_raw, metric_blk, precision=PRECISE, preferred_element_type=F32)
        fit_all = lax.all_to_all(jnp.broadcast_to(gamma_fit[None], (n_aux, dens, q_loc)), 'aux', 0, 0, tiled=True)
        fit_all = fit_all.transpose(1, 0, 2).reshape(dens, n_aux * q_loc)
        weights = jnp.einsum('dp,qp->dq', fit_all, metric_blk, precision=PRECISE, preferred_element_type=F32)
        coulomb = coulomb_part(weights, ints_blk)
        n_out = n_bas // n_aux
        coul = coulomb.reshape(dens, m_loc, n_aux, n_out).transpose(2, 0, 1, 3)
        coul = lax.all_to_all(coul, 'aux', 0, 0, tiled=True).sum(0)

        part = exchange_part(half.reshape(1).astype(jnp.int32), own, other, met)[0]
        part = part.reshape(2, n_x, m_loc, 2, n_x, 2, n_out).transpose(4, 3, 5, 1, 0, 2, 6).reshape(2 * chips, m_loc, n_out)
        got = lax.all_to_all(part, ('aux', 'x', 'core'), 0, 0, tiled=True)
        exch = got.reshape(dens, -1, m_loc, n_out).sum(1)
        return 2.0 * coul - exch

    return jax.shard_map(
        local_fock, mesh=mesh4,
        in_specs=(P(('sys', 'aux'), ('x', 'core'), None), P(('sys', 'aux'), None), P('sys', None, None)),
        out_specs=P('sys', ('x', 'core'), 'aux'), check_vma=False)
```

```python
import functools

import jax
import jax.numpy as jnp
from jax import lax
from jax.experimental import pallas as pl
from jax.experimental.pallas import tpu as pltpu
from jax.sharding import PartitionSpec as P

PRECISE = lax.Precision.HIGHEST
F32 = jnp.float32
BF16 = jnp.bfloat16
LANES = 128
NT = (((1,), (1,)), ((), ()))


def split3(x):
    hi = x.astype(BF16)
    rest = x - hi.astype(F32)
    mid = rest.astype(BF16)
    lo = (rest - mid.astype(F32)).astype(BF16)
    return hi, mid, lo


def split3_xla(x):
    hi = lax.reduce_precision(x, 8, 7)
    rest = x - hi
    mid = lax.reduce_precision(rest, 8, 7)
    return hi.astype(BF16), mid.astype(BF16), (rest - mid).astype(BF16)


def left_terms(x):
    hi, mid, lo = split3_xla(x)
    return jnp.concatenate([hi, hi, mid, hi, mid, lo], axis=-1)


def half_kernel(ints_hbm, orb_ref, dens_ref, out_ref, gam_ref, ints, wide, sems):
    q_loc, m_loc, n_bas = ints_hbm.shape
    n_col = orb_ref.shape[0]
    groups = m_loc // 8
    tiles = n_bas // LANES
    copies = [
        [pltpu.make_async_copy(
            ints_hbm.at[:, pl.ds(8 * g, 8), pl.ds(LANES * t, LANES)],
            ints.at[t, pl.ds(0, q_loc), pl.ds(8 * g, 8), :], sems.at[g, t]) for t in range(tiles)]
        for g in range(groups)]
    for group in copies:
        for copy in group:
            copy.start()
    ints[:, pl.ds(q_loc, LANES - q_loc)] = jnp.zeros((tiles, LANES - q_loc, m_loc, LANES), F32)
    flat = ints.reshape(tiles, LANES * m_loc, LANES)
    gam_ref[...] = jnp.zeros_like(gam_ref)

    for g in range(groups):
        for copy in copies[g]:
            copy.wait()

        def pair_step(j, carry, g=g):
            m = 8 * g + 2 * j
            rows = jnp.concatenate([
                jnp.concatenate([flat[t, pl.ds(m + u, LANES, stride=m_loc), :] for t in range(tiles)], axis=1)
                for u in range(2)], axis=0)
            hi, mid, lo = split3(rows)
            right = jnp.concatenate([hi, mid, hi, lo, mid, hi], axis=1)
            left = jnp.concatenate([orb_ref[...], dens_ref[4 * g + j]], axis=0)
            res = lax.dot_general(left, right, NT, preferred_element_type=F32)
            wide[pl.ds(m, n_col, stride=m_loc), :] = res[:n_col, :LANES]
            wide[pl.ds(m + 1, n_col, stride=m_loc), :] = res[:n_col, LANES:]
            gam_ref[...] += res[n_col:n_col + 8, :LANES] + res[n_col + 8:, LANES:]
            return carry

        lax.fori_loop(0, 4, pair_step, 0)

    def narrow(c, carry):
        rows = m_loc * 4
        out_ref[pl.ds(pl.multiple_of(c * rows, rows), rows), :] = wide[pl.ds(pl.multiple_of(c * rows, rows), rows), :].astype(BF16)
        return carry

    lax.fori_loop(0, n_col // 4, narrow, 0)


def half_transform(ints_blk, orb_terms, dens_terms):
    q_loc, m_loc, n_bas = ints_blk.shape
    n_col, depth = orb_terms.shape
    vmem = pl.BlockSpec(memory_space=pltpu.VMEM)
    return pl.pallas_call(
        half_kernel,
        out_shape=(jax.ShapeDtypeStruct((n_col * m_loc, LANES), BF16), jax.ShapeDtypeStruct((8, LANES), F32)),
        in_specs=[pl.BlockSpec(memory_space=pl.ANY), vmem, vmem],
        out_specs=(vmem, vmem),
        scratch_shapes=[
            pltpu.VMEM((n_bas // LANES, LANES, m_loc, LANES), F32),
            pltpu.VMEM((n_col * m_loc, LANES), F32),
            pltpu.SemaphoreType.DMA((m_loc // 8, n_bas // LANES)),
        ],
        compiler_params=pltpu.CompilerParams(vmem_limit_bytes=56 * 1024 * 1024),
        cost_estimate=pl.CostEstimate(flops=2 * 6 * n_col * n_bas * q_loc * m_loc, bytes_accessed=14 << 20, transcendentals=0),
        name='half_transform',
    )(ints_blk, orb_terms, dens_terms)


def fock_kernel(send_ref, met_ref, out_ref, own, other, fit, send_sem, recv_sem, pair_send, pair_recv):
    cols, n_src, m_loc, _ = own.shape
    n_aux, _, n_fit = met_ref.shape
    n_x = n_src // n_aux
    rows = n_x * m_loc
    tile = 256
    aux, x, core = lax.axis_index('aux'), lax.axis_index('x'), lax.axis_index('core')
    z, y = aux // 4, lax.rem(aux, 4)
    me = aux * n_x + x
    here = pl.multiple_of(core * rows, rows)
    there = pl.multiple_of((1 - core) * rows, rows)

    def send_col(c, carry):
        def send_one(k, carry):
            to_aux = lax.rem(z + k // 16, 4) * 4 + lax.rem(y + lax.rem(k // 4, 4), 4)
            to_x = lax.rem(x + lax.rem(k, 4), 4)
            pltpu.make_async_remote_copy(
                send_ref.at[to_aux * n_x + to_x, c], own.at[c, me], send_sem.at[c], recv_sem.at[c],
                device_id={'aux': to_aux, 'x': to_x}, device_id_type=pl.DeviceIdType.MESH).start()
            return carry

        return lax.fori_loop(1, n_src, send_one, carry)

    lax.fori_loop(0, cols, send_col, 0)
    for c in range(cols):
        own[c, me] = send_ref[me, c]
    out_ref[...] = jnp.zeros_like(out_ref)

    def fitted(src, c, start):
        for n in range(n_fit // tile):
            tot = None
            for s in range(n_aux // 2):
                left = jnp.concatenate([src[c, pl.ds((2 * s + t) * n_x, n_x)].reshape(rows, LANES) for t in range(2)], axis=1)
                right = met_ref[pl.ds(2 * s, 2), :, pl.ds(n * tile, tile)].reshape(2 * LANES, tile)
                part = jnp.dot(left, right, preferred_element_type=F32)
                tot = part if tot is None else tot + part
            fit[pl.ds(start, rows), pl.ds(n * tile, tile)] = tot

    def col_step(c, carry):
        got = own.at[c, pl.ds(1, n_src - 1)]
        pltpu.make_async_copy(got, got, recv_sem.at[c]).wait()
        swap = pltpu.make_async_remote_copy(
            own.at[c], other.at[c], pair_send.at[c], pair_recv.at[c],
            device_id={'core': 1 - core}, device_id_type=pl.DeviceIdType.MESH)
        swap.start()
        fitted(own, c, here)
        swap.wait()
        fitted(other, c, there)
        for n in range(n_fit // tile):
            hi, mid, lo = split3(fit[:, pl.ds(n * tile, tile)])
            same = lax.dot_general(hi, hi, NT, preferred_element_type=F32) + lax.dot_general(mid, mid, NT, preferred_element_type=F32)
            cross = lax.dot_general(hi, mid, NT, preferred_element_type=F32) + lax.dot_general(hi, lo, NT, preferred_element_type=F32)
            out_ref[0] += same
            out_ref[1] += cross
        return carry

    lax.fori_loop(0, cols, col_step, 0)
    out_ref[0] += out_ref[1] + out_ref[1].T
    for c in range(cols):
        sent = own.at[c, pl.ds(1, n_src - 1)]
        pltpu.make_async_copy(sent, sent, send_sem.at[c]).wait()


def exchange_part(send, met):
    n_src, cols, m_loc, _ = send.shape
    n_aux, _, n_fit = met.shape
    n_bas = 2 * m_loc * n_src // n_aux
    vmem = pl.BlockSpec(memory_space=pltpu.VMEM)
    return pl.pallas_call(
        fock_kernel,
        out_shape=jax.ShapeDtypeStruct((2, n_bas, n_bas), F32),
        in_specs=[vmem, vmem],
        out_specs=vmem,
        scratch_shapes=[
            pltpu.VMEM((cols, n_src, m_loc, LANES), BF16),
            pltpu.VMEM((cols, n_src, m_loc, LANES), BF16),
            pltpu.VMEM((n_bas, n_fit), F32),
            pltpu.SemaphoreType.DMA((cols,)),
            pltpu.SemaphoreType.DMA((cols,)),
            pltpu.SemaphoreType.DMA((cols,)),
            pltpu.SemaphoreType.DMA((cols,)),
        ],
        compiler_params=pltpu.CompilerParams(vmem_limit_bytes=56 * 1024 * 1024, has_side_effects=True),
        cost_estimate=pl.CostEstimate(flops=32 << 30, bytes_accessed=14 << 20, transcendentals=0),
        name='exchange_part',
    )(send, met)


def coulomb_kernel(wt_ref, ints_ref, out_ref):
    dens, q_loc = wt_ref.shape

    def q_step(q, acc):
        row = ints_ref[q]
        return tuple(acc[d] + wt_ref[d, q] * row for d in range(dens))

    acc = lax.fori_loop(0, q_loc, q_step, tuple(jnp.zeros(ints_ref.shape[1:], F32) for _ in range(dens)), unroll=4)
    for d in range(dens):
        out_ref[d] = acc[d]


def coulomb_part(weights, ints_blk):
    q_loc, m_loc, n_bas = ints_blk.shape
    dens = weights.shape[0]
    return pl.pallas_call(
        coulomb_kernel,
        grid=(m_loc // 8,),
        out_shape=jax.ShapeDtypeStruct((dens, m_loc, n_bas), F32),
        in_specs=[pl.BlockSpec(memory_space=pltpu.SMEM), pl.BlockSpec((q_loc, 8, n_bas), lambda g: (0, g, 0))],
        out_specs=pl.BlockSpec((dens, 8, n_bas), lambda g: (0, g, 0)),
        cost_estimate=pl.CostEstimate(flops=2 * dens * q_loc * m_loc * n_bas, bytes_accessed=9 << 20, transcendentals=0),
        name='coulomb_part',
    )(weights, ints_blk)


def solution(mesh):
    n_aux, n_orb = mesh.shape['aux'], mesh.shape['orb']
    n_x = n_orb // 2
    chips = n_aux * n_x
    mesh4 = jax.sharding.Mesh(mesh.devices.reshape(1, n_aux, n_x, 2), ('sys', 'aux', 'x', 'core'))

    def local_fock(ints_blk, metric_blk, orbitals):
        q_loc, m_loc, n_bas = ints_blk.shape
        dens, _, n_occ = orbitals.shape
        cols = dens * n_occ // chips
        half = lax.axis_index('core')
        orb = lax.axis_index('x') * 2 + half
        n_fit = n_bas * 0 + 1024
        met_pad = jnp.pad(metric_blk, ((0, LANES - q_loc), (0, 2 * n_fit - metric_blk.shape[1])))
        met_part = lax.dynamic_slice_in_dim(met_pad, half * n_fit, n_fit, axis=1).astype(BF16)
        met = lax.all_gather(met_part, 'aux', axis=0)

        orb_rows = lax.dynamic_slice_in_dim(orbitals, orb * m_loc, m_loc, axis=1)
        dens_rows = jnp.einsum('dmi,dli->mdl', orb_rows, orbitals, precision=PRECISE, preferred_element_type=F32)
        dens_rows = jnp.pad(dens_rows, ((0, 0), (0, 8 - dens), (0, 0))).reshape(m_loc // 2, 16, n_bas)
        orb_cols = orbitals.transpose(0, 2, 1).reshape(dens * n_occ, n_bas)
        half_tr, gamma = half_transform(ints_blk, left_terms(orb_cols), left_terms(dens_rows))

        gamma = jnp.broadcast_to(gamma[:dens][None], (2 * chips, dens, LANES))
        gamma_all = lax.all_to_all(gamma, ('aux', 'x', 'core'), 0, 0, tiled=True)

        gamma_raw = gamma_all.reshape(n_aux, n_orb, dens, LANES).sum(1)[:, :, :q_loc].transpose(1, 0, 2).reshape(dens, n_aux * q_loc)
        gamma_fit = jnp.einsum('dq,pq->dp', gamma_raw, metric_blk, precision=PRECISE, preferred_element_type=F32)
        fit_all = lax.all_to_all(jnp.broadcast_to(gamma_fit[None], (n_aux, dens, q_loc)), 'aux', 0, 0, tiled=True)
        fit_all = fit_all.transpose(1, 0, 2).reshape(dens, n_aux * q_loc)
        weights = jnp.einsum('dp,qp->dq', fit_all, metric_blk, precision=PRECISE, preferred_element_type=F32)
        coulomb = coulomb_part(weights, ints_blk)
        n_out = n_bas // n_aux
        coul = coulomb.reshape(dens, m_loc, n_aux, n_out).transpose(2, 0, 1, 3)
        coul = lax.all_to_all(coul, 'aux', 0, 0, tiled=True).sum(0)

        part = exchange_part(half_tr.reshape(chips, cols, m_loc, LANES), met)[0]
        part = part.reshape(2, n_x, m_loc, 2, n_x, 2, n_out).transpose(4, 3, 5, 1, 0, 2, 6).reshape(2 * chips, m_loc, n_out)
        got = lax.all_to_all(part, ('aux', 'x', 'core'), 0, 0, tiled=True)
        exch = got.reshape(dens, -1, m_loc, n_out).sum(1)
        return 2.0 * coul - exch

    return jax.shard_map(
        local_fock, mesh=mesh4,
        in_specs=(P(('sys', 'aux'), ('x', 'core'), None), P(('sys', 'aux'), None), P('sys', None, None)),
        out_specs=P('sys', ('x', 'core'), 'aux'), check_vma=False)
```

```python
import functools

import jax
import jax.numpy as jnp
from jax import lax
from jax.experimental import pallas as pl
from jax.experimental.pallas import tpu as pltpu
from jax.sharding import PartitionSpec as P

PRECISE = lax.Precision.HIGHEST
F32 = jnp.float32
BF16 = jnp.bfloat16
LANES = 128
NT = (((1,), (1,)), ((), ()))


def split3(x):
    hi = x.astype(BF16)
    rest = x - hi.astype(F32)
    mid = rest.astype(BF16)
    lo = (rest - mid.astype(F32)).astype(BF16)
    return hi, mid, lo


def split3_xla(x):
    hi = lax.reduce_precision(x, 8, 7)
    rest = x - hi
    mid = lax.reduce_precision(rest, 8, 7)
    return hi.astype(BF16), mid.astype(BF16), (rest - mid).astype(BF16)


def left_terms(x):
    hi, mid, lo = split3_xla(x)
    return jnp.concatenate([hi, hi, mid, hi, mid, lo], axis=-1)


def mesh_pos():
    aux = lax.axis_index('aux')
    return aux // 4, lax.rem(aux, 4), lax.axis_index('x'), lax.axis_index('core')


def peer(k):
    z, y, x, _ = mesh_pos()
    to_aux = lax.rem(z + k // 16, 4) * 4 + lax.rem(y + lax.rem(k // 4, 4), 4)
    return to_aux, lax.rem(x + lax.rem(k, 4), 4)


def push(src, dst, send_sem, recv_sem, **to):
    copy = pltpu.make_async_remote_copy(src, dst, send_sem, recv_sem, device_id=to, device_id_type=pl.DeviceIdType.MESH)
    copy.start()
    return copy


def await_bytes(like, sem):
    pltpu.make_async_copy(like, like, sem).wait()


def fock_kernel(ints_hbm, orb_ref, dens_ref, met_blk, out_ref,
                ints, wide, send, own, other, met, fit, kacc, kin, kout, kall,
                gam, gall, gsum, gpeer, gfit, gfit2, wb, jm, jt, jall,
                ints_sem, met_send, met_recv, col_send, col_recv, pair_send, pair_recv, msg_send, msg_recv):
    z, y, x, core = mesh_pos()
    aux = z * 4 + y
    n_src, cols, m_loc, _ = send.shape
    n_aux, _, n_fit = met.shape
    n_x = n_src // n_aux
    me = aux * n_x + x
    tiles, _, _, _ = ints.shape
    q_loc = ints_hbm.shape[0]
    n_col = n_src * cols
    groups = m_loc // 8
    tile = 256
    n_out = 24
    half_rows = LANES // 2

    copies = [
        [pltpu.make_async_copy(
            ints_hbm.at[:, pl.ds(8 * g, 8), pl.ds(LANES * t, LANES)],
            ints.at[t, pl.ds(0, q_loc), pl.ds(8 * g, 8), :], ints_sem.at[g, t]) for t in range(tiles)]
        for g in range(groups)]
    for group in copies:
        for copy in group:
            copy.start()
    barrier = pltpu.get_barrier_semaphore()

    def tell(k, carry):
        to_aux, to_x = peer(k)
        pl.semaphore_signal(barrier, inc=1, device_id={'aux': to_aux, 'x': to_x}, device_id_type=pl.DeviceIdType.MESH)
        return carry

    lax.fori_loop(1, n_src, tell, 0)
    pl.semaphore_signal(barrier, inc=1, device_id={'core': 1 - core}, device_id_type=pl.DeviceIdType.MESH)
    met[aux] = met_blk[:, pl.ds(pl.multiple_of(core * n_fit, n_fit), n_fit)].astype(BF16)
    ints[:, pl.ds(q_loc, LANES - q_loc)] = jnp.zeros((tiles, LANES - q_loc, m_loc, LANES), F32)
    flat = ints.reshape(tiles, LANES * m_loc, LANES)
    gam[...] = jnp.zeros_like(gam)

    upper, lower = pl.ds(0, half_rows), pl.ds(half_rows, half_rows)

    def gather_first():
        for d in range(1, 4):
            push(met.at[aux, upper], met.at[aux, upper], met_send.at[0], met_recv.at[0], aux=z * 4 + lax.rem(y + d, 4))
            push(met.at[aux, lower], met.at[aux, lower], met_send.at[1], met_recv.at[1], aux=lax.rem(z + d, 4) * 4 + y)

    def gather_second():
        three = met.at[pl.ds(0, 3), upper]
        await_bytes(three, met_recv.at[0])
        await_bytes(three, met_recv.at[1])
        for d in range(1, 4):
            for b in range(4):
                push(met.at[z * 4 + b, upper], met.at[z * 4 + b, upper], met_send.at[2], met_recv.at[2], aux=lax.rem(z + d, 4) * 4 + y)
                push(met.at[b * 4 + y, lower], met.at[b * 4 + y, lower], met_send.at[3], met_recv.at[3], aux=z * 4 + lax.rem(y + d, 4))

    for g in range(groups):
        for copy in copies[g]:
            copy.wait()

        def pair_step(j, carry, g=g):
            m = 8 * g + 2 * j
            rows = jnp.concatenate([
                jnp.concatenate([flat[t, pl.ds(m + u, LANES, stride=m_loc), :] for t in range(tiles)], axis=1)
                for u in range(2)], axis=0)
            hi, mid, lo = split3(rows)
            right = jnp.concatenate([hi, mid, hi, lo, mid, hi], axis=1)
            left = jnp.concatenate([orb_ref[...], dens_ref[4 * g + j]], axis=0)
            res = lax.dot_general(left, right, NT, preferred_element_type=F32)
            wide[pl.ds(m, n_col, stride=m_loc), :] = res[:n_col, :LANES]
            wide[pl.ds(m + 1, n_col, stride=m_loc), :] = res[:n_col, LANES:]
            gam[...] += res[n_col:n_col + 8, :LANES] + res[n_col + 8:, LANES:]
            return carry

        lax.fori_loop(0, 4, pair_step, 0)
        if g == 0:
            pl.semaphore_wait(barrier, n_src)
            gather_first()
        if g == 3:
            gather_second()

    def send_gamma(k, carry):
        to_aux, to_x = peer(k)
        push(gam, gall.at[me], msg_send.at[0], msg_recv.at[0], aux=to_aux, x=to_x)
        return carry

    lax.fori_loop(1, n_src, send_gamma, 0)
    gall[me] = gam[...]

    def send_col(c, carry):
        def narrow(k, carry):
            to_aux, to_x = peer(k)
            to = to_aux * n_x + to_x
            start = pl.multiple_of(to * (cols * m_loc) + c * m_loc, m_loc)
            send[to, c] = wide[pl.ds(start, m_loc), :].astype(BF16)
            return carry

        def send_one(k, carry):
            to_aux, to_x = peer(k)
            push(send.at[to_aux * n_x + to_x, c], own.at[c, me], col_send.at[c], col_recv.at[c], aux=to_aux, x=to_x)
            return carry

        lax.fori_loop(0, n_src, narrow, 0)
        lax.fori_loop(1, n_src, send_one, 0)
        own[c, me] = send[me, c]
        return carry

    lax.fori_loop(0, cols, send_col, 0)

    await_bytes(gall.at[pl.ds(1, n_src - 1)], msg_recv.at[0])
    for a in range(n_aux):
        gsum[a] = (gall[n_x * a] + gall[n_x * a + 1]) + (gall[n_x * a + 2] + gall[n_x * a + 3])
    push(gsum, gpeer, msg_send.at[1], msg_recv.at[1], core=1 - core).wait()
    twelve = met.at[pl.ds(0, 12), upper]
    await_bytes(twelve, met_recv.at[2])
    await_bytes(twelve, met_recv.at[3])
    tot = None
    for s in range(n_aux // 2):
        pair = jnp.concatenate([gsum[2 * s + t] + gpeer[2 * s + t] for t in range(2)], axis=1)
        hi, mid, lo = (v.astype(F32) for v in split3(pair))
        left = jnp.concatenate([hi, mid, lo, jnp.zeros_like(hi)], axis=0).astype(BF16)
        part = jnp.dot(left, met[pl.ds(2 * s, 2)].reshape(2 * LANES, n_fit), preferred_element_type=F32)
        tot = part if tot is None else tot + part
    gfit[...] = tot[0:8] + tot[8:16] + tot[16:24]
    push(gfit, gfit2, msg_send.at[2], msg_recv.at[2], core=1 - core).wait()
    low = jnp.where(core == 0, gfit[...], gfit2[...])
    high = jnp.where(core == 0, gfit2[...], gfit[...])
    wts = lax.dot_general(met_blk[...], jnp.concatenate([low, high], axis=1), NT, precision=PRECISE, preferred_element_type=F32)
    dens = wb.shape[0]
    for d in range(dens):
        wb[d] = jnp.broadcast_to(wts[:, d:d + 1], (LANES, LANES))
    jm[...] = jnp.zeros_like(jm)

    def coul_group(g, carry):
        def q_step(q, acc):
            rows = [ints[t, q, pl.ds(pl.multiple_of(8 * g, 8), 8), :] for t in range(tiles)]
            return tuple(acc[d * tiles + t] + wb[d, pl.ds(q, 1), :] * rows[t] for d in range(dens) for t in range(tiles))

        acc = lax.fori_loop(0, q_loc, q_step, tuple(jnp.zeros((8, LANES), F32) for _ in range(dens * tiles)), unroll=4)
        for d in range(dens):
            for t in range(tiles):
                jm[d // 2, pl.ds(pl.multiple_of((d % 2) * half_rows + 8 * g, 8), 8), pl.ds(LANES * t, LANES)] = acc[d * tiles + t]
        return carry

    lax.fori_loop(0, groups, coul_group, 0)
    for p in range(dens // 2):
        jt[p] = jm[p].T

    def send_coul(k, carry):
        to_aux = lax.rem(z + k // 4, 4) * 4 + lax.rem(y + lax.rem(k, 4), 4)
        push(jt.at[:, pl.ds(pl.multiple_of(to_aux * n_out, 8), n_out), :], jall.at[aux], msg_send.at[3], msg_recv.at[3], aux=to_aux)
        return carry

    lax.fori_loop(1, n_aux, send_coul, 0)
    jall[aux] = jt[:, pl.ds(pl.multiple_of(aux * n_out, 8), n_out), :]

    fit[...] = jnp.zeros_like(fit)
    kacc[...] = jnp.zeros_like(kacc)
    pad_rows = 64

    def fitted(src, c, side):
        rows = n_x * m_loc
        for n in range(n_fit // tile):
            tot = None
            for s in range(n_aux // 2):
                left = jnp.concatenate([src[c, pl.ds((2 * s + t) * n_x, n_x)].reshape(rows, LANES) for t in range(2)], axis=1)
                right = met[pl.ds(2 * s, 2), :, pl.ds(n * tile, tile)].reshape(2 * LANES, tile)
                part = jnp.dot(left, right, preferred_element_type=F32)
                tot = part if tot is None else tot + part
            for b in range(n_x):
                start = pl.multiple_of((side * n_x + b) * pad_rows, pad_rows)
                fit[pl.ds(start, m_loc), pl.ds(n * tile, tile)] = tot[b * m_loc:(b + 1) * m_loc]

    def col_step(c, carry):
        await_bytes(own.at[c, pl.ds(1, n_src - 1)], col_recv.at[c])
        swap = push(own.at[c], other.at[c], pair_send.at[c], pair_recv.at[c], core=1 - core)
        fitted(own, c, core)
        swap.wait()
        fitted(other, c, 1 - core)
        for n in range(n_fit // tile):
            hi, mid, lo = split3(fit[:, pl.ds(n * tile, tile)])
            short = [jnp.concatenate([v[pad_rows * b:pad_rows * b + m_loc] for b in range(2 * n_x)], axis=0) for v in (hi, mid, lo)]
            left = jnp.concatenate([short[0], short[0], short[1], short[0], short[1], short[2]], axis=1)
            right = jnp.concatenate([hi, mid, hi, lo, mid, hi], axis=1)
            kacc[...] += lax.dot_general(left, right, NT, preferred_element_type=F32)
        return carry

    lax.fori_loop(0, cols, col_step, 0)

    width = n_x * pad_rows
    mine = pl.multiple_of(core * width, width)
    theirs = pl.multiple_of((1 - core) * width, width)
    push(kacc.at[:, pl.ds(theirs, width)], kin, msg_send.at[4], msg_recv.at[4], core=1 - core).wait()
    ksum = kacc[:, pl.ds(mine, width)] + kin[...]
    for t in range(width // LANES):
        kout[t] = ksum[:, t * LANES:(t + 1) * LANES]

    def rows_of(to_aux):
        start = lax.rem(to_aux // 2, 2) * (n_x * m_loc) + to_aux // 4 * m_loc + lax.rem(to_aux, 2) * n_out
        return pl.ds(pl.multiple_of(start, 8), n_out)

    def send_exch(k, carry):
        to_aux, to_x = peer(k)
        push(kout.at[to_x // 2, rows_of(to_aux)], kall.at[me], msg_send.at[5], msg_recv.at[5], aux=to_aux, x=to_x)
        return carry

    lax.fori_loop(1, n_src, send_exch, 0)
    kall[me] = kout[x // 2, rows_of(aux)]
    await_bytes(jall.at[pl.ds(1, n_aux - 1)], msg_recv.at[3])
    await_bytes(kall.at[pl.ds(1, n_src - 1)], msg_recv.at[5])
    per = n_src // dens
    for d in range(dens):
        coul = jall[0, d // 2]
        for a in range(1, n_aux):
            coul = coul + jall[a, d // 2]
        coul = pltpu.roll(coul, half_rows, 1) if d % 2 else coul
        exch = kall[per * d]
        for i in range(1, per):
            exch = exch + kall[per * d + i]
        exch = jnp.where(lax.rem(x, 2) == 1, pltpu.roll(exch, half_rows, 1), exch)
        out_ref[d] = 2.0 * coul - exch

    for c in range(cols):
        await_bytes(own.at[c, pl.ds(1, n_src - 1)], col_send.at[c])
    await_bytes(gall.at[pl.ds(1, n_src - 1)], msg_send.at[0])
    await_bytes(jall.at[pl.ds(1, n_aux - 1)], msg_send.at[3])
    await_bytes(kall.at[pl.ds(1, n_src - 1)], msg_send.at[5])
    for i, n in enumerate((3, 3, 12, 12)):
        await_bytes(met.at[pl.ds(0, n), upper], met_send.at[i])


def fock_build(ints_blk, orb_terms, dens_terms, met_blk, n_aux, dens):
    q_loc, m_loc, n_bas = ints_blk.shape
    n_col = orb_terms.shape[0]
    n_x = n_bas // m_loc // 2
    chips = n_aux * n_x
    cols = n_col // chips
    n_fit = met_blk.shape[1] // 2
    n_out = n_bas // n_aux
    tiles = n_bas // LANES
    vmem = pl.BlockSpec(memory_space=pltpu.VMEM)
    dma = pltpu.SemaphoreType.DMA
    return pl.pallas_call(
        fock_kernel,
        out_shape=jax.ShapeDtypeStruct((dens, n_out, LANES), F32),
        in_specs=[pl.BlockSpec(memory_space=pl.ANY), vmem, vmem, vmem],
        out_specs=vmem,
        scratch_shapes=[
            pltpu.VMEM((tiles, LANES, m_loc, LANES), F32),
            pltpu.VMEM((n_col * m_loc, LANES), F32),
            pltpu.VMEM((chips, cols, m_loc, LANES), BF16),
            pltpu.VMEM((cols, chips, m_loc, LANES), BF16),
            pltpu.VMEM((cols, chips, m_loc, LANES), BF16),
            pltpu.VMEM((n_aux, LANES, n_fit), BF16),
            pltpu.VMEM((2 * n_x * 64, n_fit), F32),
            pltpu.VMEM((n_bas, 2 * n_x * 64), F32),
            pltpu.VMEM((n_bas, n_x * 64), F32),
            pltpu.VMEM((n_x // 2, n_bas, LANES), F32),
            pltpu.VMEM((chips, n_out, LANES), F32),
            pltpu.VMEM((8, LANES), F32),
            pltpu.VMEM((chips, 8, LANES), F32),
            pltpu.VMEM((n_aux, 8, LANES), F32),
            pltpu.VMEM((n_aux, 8, LANES), F32),
            pltpu.VMEM((8, n_fit), F32),
            pltpu.VMEM((8, n_fit), F32),
            pltpu.VMEM((dens, LANES, LANES), F32),
            pltpu.VMEM((dens // 2, LANES, n_bas), F32),
            pltpu.VMEM((dens // 2, n_bas, LANES), F32),
            pltpu.VMEM((n_aux, dens // 2, n_out, LANES), F32),
            dma((m_loc // 8, tiles)), dma((4,)), dma((4,)), dma((cols,)), dma((cols,)), dma((cols,)), dma((cols,)), dma((6,)), dma((6,)),
        ],
        compiler_params=pltpu.CompilerParams(vmem_limit_bytes=62 * 1024 * 1024, collective_id=0, has_side_effects=True),
        name='fock_build',
    )(ints_blk, orb_terms, dens_terms, met_blk)


def solution(mesh):
    n_aux, n_orb = mesh.shape['aux'], mesh.shape['orb']
    mesh4 = jax.sharding.Mesh(mesh.devices.reshape(1, n_aux, n_orb // 2, 2), ('sys', 'aux', 'x', 'core'))

    def local_fock(ints_blk, metric_blk, orbitals):
        q_loc, m_loc, n_bas = ints_blk.shape
        dens, _, n_occ = orbitals.shape
        orb = lax.axis_index('x') * 2 + lax.axis_index('core')
        met_pad = jnp.pad(metric_blk, ((0, LANES - q_loc), (0, -metric_blk.shape[1] % 512)))
        orb_rows = lax.dynamic_slice_in_dim(orbitals, orb * m_loc, m_loc, axis=1)
        dens_rows = jnp.einsum('dmi,dli->mdl', orb_rows, orbitals, precision=PRECISE, preferred_element_type=F32)
        dens_rows = jnp.pad(dens_rows, ((0, 0), (0, 8 - dens), (0, 0))).reshape(m_loc // 2, 16, n_bas)
        orb_cols = orbitals.transpose(0, 2, 1).reshape(dens * n_occ, n_bas)
        out = fock_build(ints_blk, left_terms(orb_cols), left_terms(dens_rows), met_pad, n_aux, dens)
        return out[:, :, :m_loc].transpose(0, 2, 1)

    return jax.shard_map(
        local_fock, mesh=mesh4,
        in_specs=(P(('sys', 'aux'), ('x', 'core'), None), P(('sys', 'aux'), None), P('sys', None, None)),
        out_specs=P('sys', ('x', 'core'), 'aux'), check_vma=False)
```

```python
import functools

import jax
import jax.numpy as jnp
from jax import lax
from jax.experimental import pallas as pl
from jax.experimental.pallas import tpu as pltpu
from jax.sharding import PartitionSpec as P

PRECISE = lax.Precision.HIGHEST
F32 = jnp.float32
BF16 = jnp.bfloat16
LANES = 128
NT = (((1,), (1,)), ((), ()))


def split3(x):
    hi = x.astype(BF16)
    rest = x - hi.astype(F32)
    mid = rest.astype(BF16)
    lo = (rest - mid.astype(F32)).astype(BF16)
    return hi, mid, lo


def mesh_pos():
    aux = lax.axis_index('aux')
    return aux // 4, lax.rem(aux, 4), lax.axis_index('x'), lax.axis_index('core')


def near():
    z, y, x, _ = mesh_pos()
    return [[lax.rem(p + d, 4) for d in range(4)] for p in (z, y, x)]


def batch(zs, ys, xs, b):
    for dy in range(4):
        for dx in range(4):
            dz = (b + dy + dx) % 4
            if dz or dy or dx:
                yield zs[dz] * 4 + ys[dy], xs[dx]


def push(src, dst, send_sem, recv_sem, **to):
    copy = pltpu.make_async_remote_copy(src, dst, send_sem, recv_sem, device_id=to, device_id_type=pl.DeviceIdType.MESH)
    copy.start()
    return copy


def await_bytes(like, sem):
    pltpu.make_async_copy(like, like, sem).wait()


def fock_kernel(ints_hbm, orb_ref, dens_ref, met_ref, out_ref,
                ints, wide, terms, met_blk, send, own, other, met, fit, kacc, kin, kout, kall,
                gam, gall, gsum, gpeer, gfit, fall, wb, jm, jt, jall,
                ints_sem, met_send, met_recv, col_send, col_recv, pair_send, pair_recv, msg_send, msg_recv):
    z, y, x, core = mesh_pos()
    zs, ys, xs = near()
    aux = z * 4 + y
    n_src, cols, m_loc, _ = send.shape
    n_aux, _, n_fit = met.shape
    n_x = n_src // n_aux
    me = aux * n_x + x
    tiles, _, m_pad, _ = ints.shape
    q_loc = ints_hbm.shape[0]
    skip = wide.shape[0] // (n_src * cols)
    n_col = n_src * cols
    groups = m_loc // 8
    tile = 256
    n_out = 24
    half_rows = LANES // 2

    copies = [
        [pltpu.make_async_copy(
            ints_hbm.at[:, pl.ds(8 * g, 8), pl.ds(LANES * t, LANES)],
            ints.at[t, pl.ds(0, q_loc), pl.ds(8 * g, 8), :], ints_sem.at[g, t]) for t in range(tiles)]
        for g in range(groups)]
    for group in copies:
        for copy in group:
            copy.start()
    barrier = pltpu.get_barrier_semaphore()

    for b in range(4):
        for to_aux, to_x in batch(zs, ys, xs, b):
            pl.semaphore_signal(barrier, inc=1, device_id={'aux': to_aux, 'x': to_x}, device_id_type=pl.DeviceIdType.MESH)
    pl.semaphore_signal(barrier, inc=1, device_id={'core': 1 - core}, device_id_type=pl.DeviceIdType.MESH)
    met_blk[...] = jnp.zeros_like(met_blk)
    for b in range(n_aux):
        met_blk[pl.ds(0, q_loc), pl.ds(b * LANES, q_loc)] = met_ref[:, b * q_loc:(b + 1) * q_loc]
    met[aux] = met_blk[:, pl.ds(pl.multiple_of(core * n_fit, n_fit), n_fit)].astype(BF16)
    ints[:, pl.ds(q_loc, LANES - q_loc)] = jnp.zeros((tiles, LANES - q_loc, m_pad, LANES), F32)
    flat = ints.reshape(tiles, LANES * m_pad, LANES)
    for i, term in enumerate(split3(orb_ref[...])):
        terms[i] = term
    gam[...] = jnp.zeros_like(gam)

    upper, lower = pl.ds(0, half_rows), pl.ds(half_rows, half_rows)

    def gather_first():
        for d in range(1, 4):
            push(met.at[aux, upper], met.at[aux, upper], met_send.at[0], met_recv.at[0], aux=z * 4 + ys[d])
            push(met.at[aux, lower], met.at[aux, lower], met_send.at[1], met_recv.at[1], aux=zs[d] * 4 + y)

    def gather_second():
        three = met.at[pl.ds(0, 3), upper]
        await_bytes(three, met_recv.at[0])
        await_bytes(three, met_recv.at[1])
        for d in range(1, 4):
            for b in range(4):
                push(met.at[z * 4 + b, upper], met.at[z * 4 + b, upper], met_send.at[2], met_recv.at[2], aux=zs[d] * 4 + y)
                push(met.at[b * 4 + y, lower], met.at[b * 4 + y, lower], met_send.at[3], met_recv.at[3], aux=z * 4 + ys[d])

    for g in range(groups):
        for copy in copies[g]:
            copy.wait()

        def pair_step(j, carry, g=g):
            m = 8 * g + 2 * j
            rows = jnp.concatenate([
                jnp.concatenate([flat[t, pl.ds(m + u, LANES, stride=m_pad), :] for t in range(tiles)], axis=1)
                for u in range(2)], axis=0)
            hi, mid, lo = split3(rows)
            right = jnp.concatenate([hi, mid, hi, lo, mid, hi], axis=1)
            both = [jnp.concatenate([terms[i], v], axis=0) for i, v in enumerate(split3(dens_ref[4 * g + j]))]
            left = jnp.concatenate([both[0], both[0], both[1], both[0], both[1], both[2]], axis=1)
            res = lax.dot_general(left, right, NT, preferred_element_type=F32)
            wide[pl.ds(m, n_col, stride=skip), :] = res[:n_col, :LANES]
            wide[pl.ds(m + 1, n_col, stride=skip), :] = res[:n_col, LANES:]
            gam[...] += res[n_col:n_col + 8, :LANES] + res[n_col + 8:, LANES:]
            return carry

        lax.fori_loop(0, 4, pair_step, 0)
        if g == 0:
            pl.semaphore_wait(barrier, n_src)
            gather_first()
        if g == 3:
            gather_second()

    def narrow(c):
        def one(to, carry):
            send[to, c] = wide[pl.ds((to * cols + c) * skip, m_loc), :].astype(BF16)
            return carry

        lax.fori_loop(0, n_src, one, 0, unroll=4)

    def send_batch(c, b):
        for to_aux, to_x in batch(zs, ys, xs, b):
            push(send.at[to_aux * n_x + to_x, c], own.at[c, me], col_send.at[c], col_recv.at[c], aux=to_aux, x=to_x)

    narrow(0)
    for b in range(4):
        for to_aux, to_x in batch(zs, ys, xs, b):
            push(gam, gall.at[me], msg_send.at[0], msg_recv.at[0], aux=to_aux, x=to_x)
    gall[me] = gam[...]
    for b in range(4):
        send_batch(0, b)
    for c in range(1, cols):
        narrow(c)
    for c in range(cols):
        own[c, me] = send[me, c]

    await_bytes(gall.at[pl.ds(1, n_src - 1)], msg_recv.at[0])
    for a in range(n_aux):
        gsum[a] = (gall[n_x * a] + gall[n_x * a + 1]) + (gall[n_x * a + 2] + gall[n_x * a + 3])
    swap = push(gsum, gpeer, msg_send.at[1], msg_recv.at[1], core=1 - core)
    send_batch(1, 0)
    send_batch(1, 1)
    swap.wait()

    def times_met(blocks):
        return lax.dot_general(jnp.concatenate(blocks, axis=1), met_blk[...], NT, precision=PRECISE, preferred_element_type=F32)

    gfit[...] = times_met([gsum[a] + gpeer[a] for a in range(n_aux)])
    for dz in range(4):
        for dy in range(4):
            if dz or dy:
                push(gfit, fall.at[aux], msg_send.at[2], msg_recv.at[2], aux=zs[dz] * 4 + ys[dy])
    fall[aux] = gfit[...]
    send_batch(1, 2)
    send_batch(1, 3)
    await_bytes(fall.at[pl.ds(1, n_aux - 1)], msg_recv.at[2])
    wts = lax.dot_general(met_blk[...], jnp.concatenate([fall[a] for a in range(n_aux)], axis=1), NT, precision=PRECISE, preferred_element_type=F32)
    dens = wb.shape[0]
    for d in range(dens):
        wb[d] = jnp.broadcast_to(wts[:, d:d + 1], (LANES, LANES))
    jm[...] = jnp.zeros_like(jm)

    def coul_group(g, carry):
        def q_step(q, acc):
            rows = [ints[t, q, pl.ds(pl.multiple_of(8 * g, 8), 8), :] for t in range(tiles)]
            return tuple(acc[d * tiles + t] + wb[d, pl.ds(q, 1), :] * rows[t] for d in range(dens) for t in range(tiles))

        acc = lax.fori_loop(0, q_loc, q_step, tuple(jnp.zeros((8, LANES), F32) for _ in range(dens * tiles)), unroll=4)
        for d in range(dens):
            for t in range(tiles):
                jm[d // 2, pl.ds(pl.multiple_of((d % 2) * half_rows + 8 * g, 8), 8), pl.ds(LANES * t, LANES)] = acc[d * tiles + t]
        return carry

    for b in range(2):
        lax.fori_loop(b * groups // 2, (b + 1) * groups // 2, coul_group, 0)
        send_batch(2, 2 * b)
        send_batch(2, 2 * b + 1)
    for p in range(dens // 2):
        jt[p] = jm[p].T

    for dz in range(4):
        for dy in range(4):
            if dz or dy:
                to_aux = zs[dz] * 4 + ys[dy]
                push(jt.at[:, pl.ds(pl.multiple_of(to_aux * n_out, 8), n_out), :], jall.at[aux], msg_send.at[3], msg_recv.at[3], aux=to_aux)
    jall[aux] = jt[:, pl.ds(pl.multiple_of(aux * n_out, 8), n_out), :]

    fit[...] = jnp.zeros_like(fit)
    kacc[...] = jnp.zeros_like(kacc)
    pad_rows = 64

    def fitted(src, c, side):
        rows = n_x * m_loc
        for n in range(n_fit // tile):
            tot = None
            for s in range(n_aux // 2):
                left = jnp.concatenate([src[c, pl.ds((2 * s + t) * n_x, n_x)].reshape(rows, LANES) for t in range(2)], axis=1)
                right = met[pl.ds(2 * s, 2), :, pl.ds(n * tile, tile)].reshape(2 * LANES, tile)
                part = jnp.dot(left, right, preferred_element_type=F32)
                tot = part if tot is None else tot + part
            for b in range(n_x):
                start = pl.multiple_of((side * n_x + b) * pad_rows, pad_rows)
                fit[pl.ds(start, m_loc), pl.ds(n * tile, tile)] = tot[b * m_loc:(b + 1) * m_loc]

    twelve = met.at[pl.ds(0, 12), upper]
    await_bytes(twelve, met_recv.at[2])
    await_bytes(twelve, met_recv.at[3])

    def col_step(c, carry):
        def more(b):
            @pl.when(c < cols - 3)
            def _():
                send_batch(c + 3, b)

        more(0)
        await_bytes(own.at[c, pl.ds(1, n_src - 1)], col_recv.at[c])
        swap = push(own.at[c], other.at[c], pair_send.at[c], pair_recv.at[c], core=1 - core)
        fitted(own, c, core)
        more(1)
        swap.wait()
        fitted(other, c, 1 - core)
        more(2)
        for n in range(n_fit // tile):
            hi, mid, lo = split3(fit[:, pl.ds(n * tile, tile)])
            short = [jnp.concatenate([v[pad_rows * b:pad_rows * b + m_loc] for b in range(2 * n_x)], axis=0) for v in (hi, mid, lo)]
            left = jnp.concatenate([short[0], short[0], short[1], short[0], short[1], short[2]], axis=1)
            right = jnp.concatenate([hi, mid, hi, lo, mid, hi], axis=1)
            kacc[...] += lax.dot_general(left, right, NT, preferred_element_type=F32)
            if n == 1:
                more(3)
        return carry

    lax.fori_loop(0, cols, col_step, 0)

    width = n_x * pad_rows
    mine = pl.multiple_of(core * width, width)
    theirs = pl.multiple_of((1 - core) * width, width)
    push(kacc.at[:, pl.ds(theirs, width)], kin, msg_send.at[4], msg_recv.at[4], core=1 - core).wait()
    ksum = kacc[:, pl.ds(mine, width)] + kin[...]
    for t in range(width // LANES):
        kout[t] = ksum[:, t * LANES:(t + 1) * LANES]

    def rows_of(to_aux):
        start = lax.rem(to_aux // 2, 2) * (n_x * m_loc) + to_aux // 4 * m_loc + lax.rem(to_aux, 2) * n_out
        return pl.ds(pl.multiple_of(start, 8), n_out)

    for b in range(4):
        for to_aux, to_x in batch(zs, ys, xs, b):
            push(kout.at[to_x // 2, rows_of(to_aux)], kall.at[me], msg_send.at[5], msg_recv.at[5], aux=to_aux, x=to_x)
    kall[me] = kout[x // 2, rows_of(aux)]
    await_bytes(jall.at[pl.ds(1, n_aux - 1)], msg_recv.at[3])
    await_bytes(kall.at[pl.ds(1, n_src - 1)], msg_recv.at[5])
    per = n_src // dens
    for d in range(dens):
        coul = jall[0, d // 2]
        for a in range(1, n_aux):
            coul = coul + jall[a, d // 2]
        coul = pltpu.roll(coul, half_rows, 1) if d % 2 else coul
        exch = kall[per * d]
        for i in range(1, per):
            exch = exch + kall[per * d + i]
        exch = jnp.where(lax.rem(x, 2) == 1, pltpu.roll(exch, half_rows, 1), exch)
        out_ref[d] = 2.0 * coul - exch

    for c in range(cols):
        await_bytes(own.at[c, pl.ds(1, n_src - 1)], col_send.at[c])
    await_bytes(gall.at[pl.ds(1, n_src - 1)], msg_send.at[0])
    await_bytes(fall.at[pl.ds(1, n_aux - 1)], msg_send.at[2])
    await_bytes(jall.at[pl.ds(1, n_aux - 1)], msg_send.at[3])
    await_bytes(kall.at[pl.ds(1, n_src - 1)], msg_send.at[5])
    for i, n in enumerate((3, 3, 12, 12)):
        await_bytes(met.at[pl.ds(0, n), upper], met_send.at[i])


def fock_build(ints_blk, orb_cols, dens_rows, metric_blk, n_aux, dens):
    q_loc, m_loc, n_bas = ints_blk.shape
    n_col = orb_cols.shape[0]
    n_x = n_bas // m_loc // 2
    chips = n_aux * n_x
    cols = n_col // chips
    n_fit = n_aux // 2 * LANES
    n_out = n_bas // n_aux
    tiles = n_bas // LANES
    vmem = pl.BlockSpec(memory_space=pltpu.VMEM)
    dma = pltpu.SemaphoreType.DMA
    return pl.pallas_call(
        fock_kernel,
        out_shape=jax.ShapeDtypeStruct((dens, n_out, LANES), F32),
        in_specs=[pl.BlockSpec(memory_space=pl.ANY), vmem, vmem, vmem],
        out_specs=vmem,
        scratch_shapes=[
            pltpu.VMEM((tiles, LANES, m_loc + 8, LANES), F32),
            pltpu.VMEM((n_col * (m_loc + 1), LANES), F32),
            pltpu.VMEM((3, n_col, n_bas), BF16),
            pltpu.VMEM((LANES, 2 * n_fit), F32),
            pltpu.VMEM((chips, cols, m_loc, LANES), BF16),
            pltpu.VMEM((cols, chips, m_loc, LANES), BF16),
            pltpu.VMEM((cols, chips, m_loc, LANES), BF16),
            pltpu.VMEM((n_aux, LANES, n_fit), BF16),
            pltpu.VMEM((2 * n_x * 64, n_fit), F32),
            pltpu.VMEM((n_bas, 2 * n_x * 64), F32),
            pltpu.VMEM((n_bas, n_x * 64), F32),
            pltpu.VMEM((n_x // 2, n_bas, LANES), F32),
            pltpu.VMEM((chips, n_out, LANES), F32),
            pltpu.VMEM((8, LANES), F32),
            pltpu.VMEM((chips, 8, LANES), F32),
            pltpu.VMEM((n_aux, 8, LANES), F32),
            pltpu.VMEM((n_aux, 8, LANES), F32),
            pltpu.VMEM((8, LANES), F32),
            pltpu.VMEM((n_aux, 8, LANES), F32),
            pltpu.VMEM((dens, LANES, LANES), F32),
            pltpu.VMEM((dens // 2, LANES, n_bas), F32),
            pltpu.VMEM((dens // 2, n_bas, LANES), F32),
            pltpu.VMEM((n_aux, dens // 2, n_out, LANES), F32),
            dma((m_loc // 8, tiles)), dma((4,)), dma((4,)), dma((cols,)), dma((cols,)), dma((cols,)), dma((cols,)), dma((6,)), dma((6,)),
        ],
        compiler_params=pltpu.CompilerParams(vmem_limit_bytes=62 * 1024 * 1024, collective_id=0, has_side_effects=True),
        name='fock_build',
    )(ints_blk, orb_cols, dens_rows, metric_blk)


def solution(mesh):
    n_aux, n_orb = mesh.shape['aux'], mesh.shape['orb']
    mesh4 = jax.sharding.Mesh(mesh.devices.reshape(1, n_aux, n_orb // 2, 2), ('sys', 'aux', 'x', 'core'))

    def local_fock(ints_blk, metric_blk, orbitals):
        q_loc, m_loc, n_bas = ints_blk.shape
        dens, _, n_occ = orbitals.shape
        orb = lax.axis_index('x') * 2 + lax.axis_index('core')
        orb_rows = lax.dynamic_slice_in_dim(orbitals, orb * m_loc, m_loc, axis=1)
        dens_rows = jnp.einsum('dmi,dli->mdl', orb_rows, orbitals, precision=PRECISE, preferred_element_type=F32)
        dens_rows = jnp.pad(dens_rows, ((0, 0), (0, 8 - dens), (0, 0))).reshape(m_loc // 2, 16, n_bas)
        orb_cols = orbitals.transpose(0, 2, 1).reshape(dens * n_occ, n_bas)
        out = fock_build(ints_blk, orb_cols, dens_rows, metric_blk, n_aux, dens)
        return out[:, :, :m_loc].transpose(0, 2, 1)

    return jax.shard_map(
        local_fock, mesh=mesh4,
        in_specs=(P(('sys', 'aux'), ('x', 'core'), None), P(('sys', 'aux'), None), P('sys', None, None)),
        out_specs=P('sys', ('x', 'core'), 'aux'), check_vma=False)
```

```python
import functools

import jax
import jax.numpy as jnp
from jax import lax
from jax.experimental import pallas as pl
from jax.experimental.pallas import tpu as pltpu
from jax.sharding import PartitionSpec as P

PRECISE = lax.Precision.HIGHEST
F32 = jnp.float32
BF16 = jnp.bfloat16
LANES = 128
NT = (((1,), (1,)), ((), ()))


def split3(x):
    hi = x.astype(BF16)
    rest = x - hi.astype(F32)
    mid = rest.astype(BF16)
    lo = (rest - mid.astype(F32)).astype(BF16)
    return hi, mid, lo


def mesh_pos():
    aux = lax.axis_index('aux')
    return aux // 4, lax.rem(aux, 4), lax.axis_index('x'), lax.axis_index('core')


def near():
    z, y, x, _ = mesh_pos()
    return [[lax.rem(p + d, 4) for d in range(4)] for p in (z, y, x)]


def batch(zs, ys, xs, b):
    for dy in range(4):
        for dx in range(4):
            dz = (b + dy + dx) % 4
            if dz or dy or dx:
                yield zs[dz] * 4 + ys[dy], xs[dx]


def push(src, dst, send_sem, recv_sem, **to):
    copy = pltpu.make_async_remote_copy(src, dst, send_sem, recv_sem, device_id=to, device_id_type=pl.DeviceIdType.MESH)
    copy.start()
    return copy


def await_bytes(like, sem):
    pltpu.make_async_copy(like, like, sem).wait()


def fock_kernel(ints_hbm, orb_ref, met_ref, out_ref,
                ints, wide, terms, drows, met_blk, send, own, other, met, fit, kacc, kin, kpk, kall,
                gam, gall, gsum, gpeer, gfit, fall, wb, jm, jt, jall,
                ints_sem, met_send, met_recv, col_send, col_recv, pair_send, pair_recv, msg_send, msg_recv):
    z, y, x, core = mesh_pos()
    zs, ys, xs = near()
    aux = z * 4 + y
    n_src, cols, m_loc, _ = send.shape
    n_aux, _, n_fit = met.shape
    n_x = n_src // n_aux
    me = aux * n_x + x
    tiles, _, m_pad, _ = ints.shape
    q_loc = ints_hbm.shape[0]
    skip = wide.shape[0] // (n_src * cols)
    n_col = n_src * cols
    groups = m_loc // 8
    tile = 256
    n_out = 24
    half_rows = LANES // 2

    copies = [
        [pltpu.make_async_copy(
            ints_hbm.at[:, pl.ds(8 * g, 8), pl.ds(LANES * t, LANES)],
            ints.at[t, pl.ds(0, q_loc), pl.ds(8 * g, 8), :], ints_sem.at[g, t]) for t in range(tiles)]
        for g in range(groups)]
    for group in copies:
        for copy in group:
            copy.start()
    barrier = pltpu.get_barrier_semaphore()

    for b in range(4):
        for to_aux, to_x in batch(zs, ys, xs, b):
            pl.semaphore_signal(barrier, inc=1, device_id={'aux': to_aux, 'x': to_x}, device_id_type=pl.DeviceIdType.MESH)
    pl.semaphore_signal(barrier, inc=1, device_id={'core': 1 - core}, device_id_type=pl.DeviceIdType.MESH)
    met_blk[...] = jnp.zeros_like(met_blk)
    for b in range(n_aux):
        met_blk[pl.ds(0, q_loc), pl.ds(b * LANES, q_loc)] = met_ref[:, b * q_loc:(b + 1) * q_loc]
    met[aux] = met_blk[:, pl.ds(pl.multiple_of(core * n_fit, n_fit), n_fit)].astype(BF16)
    ints[:, pl.ds(q_loc, LANES - q_loc)] = jnp.zeros((tiles, LANES - q_loc, m_pad, LANES), F32)
    flat = ints.reshape(tiles, LANES * m_pad, LANES)
    dens, _, n_occ = orb_ref.shape
    drows[...] = jnp.zeros_like(drows)
    for d in range(dens):
        for i, term in enumerate(split3(orb_ref[d].T)):
            terms[i, pl.ds(d * n_occ, n_occ), :] = term
        here = orb_ref[d, pl.ds(pl.multiple_of((x * 2 + core) * m_loc, m_loc), m_loc), :]
        full = lax.dot_general(here, orb_ref[d], NT, precision=PRECISE, preferred_element_type=F32)
        for t in range(tiles):
            drows[t, pl.ds(d, m_loc, stride=8), :] = full[:, t * LANES:(t + 1) * LANES]
    gam[...] = jnp.zeros_like(gam)

    upper, lower = pl.ds(0, half_rows), pl.ds(half_rows, half_rows)

    def to_y(d, blk, half, n):
        push(met.at[blk, half], met.at[blk, half], met_send.at[n], met_recv.at[n], aux=z * 4 + ys[d])

    def to_z(d, blk, half, n):
        push(met.at[blk, half], met.at[blk, half], met_send.at[n], met_recv.at[n], aux=zs[d] * 4 + y)

    def gather_first():
        for d in (1, 3, 2):
            to_y(d, aux, upper, 0)
            to_z(d, aux, lower, 1)
        for d in (1, 3, 2):
            to_z(d, aux, upper, 2)
            to_y(d, aux, lower, 3)

    def gather_second():
        three = met.at[pl.ds(0, 3), upper]
        await_bytes(three, met_recv.at[0])
        await_bytes(three, met_recv.at[1])
        for b in range(1, 4):
            for d in (1, 3, 2):
                to_z(d, z * 4 + ys[b], upper, 2)
                to_y(d, zs[b] * 4 + y, lower, 3)

    pl.semaphore_wait(barrier, n_src)
    gather_first()
    for g in range(groups):
        for copy in copies[g]:
            copy.wait()

        def pair_step(j, carry, g=g):
            m = 8 * g + 2 * j
            rows = jnp.concatenate([
                jnp.concatenate([flat[t, pl.ds(m + u, LANES, stride=m_pad), :] for t in range(tiles)], axis=1)
                for u in range(2)], axis=0)
            hi, mid, lo = split3(rows)
            right = jnp.concatenate([hi, mid, hi, lo, mid, hi], axis=1)
            at = pl.ds(pl.multiple_of(16 * (4 * g + j), 16), 16)
            drow = jnp.concatenate([drows[t, at, :] for t in range(tiles)], axis=1)
            both = [jnp.concatenate([terms[i], v], axis=0) for i, v in enumerate(split3(drow))]
            left = jnp.concatenate([both[0], both[0], both[1], both[0], both[1], both[2]], axis=1)
            res = lax.dot_general(left, right, NT, preferred_element_type=F32)
            wide[pl.ds(m, n_col, stride=skip), :] = res[:n_col, :LANES]
            wide[pl.ds(m + 1, n_col, stride=skip), :] = res[:n_col, LANES:]
            gam[...] += res[n_col:n_col + 8, :LANES] + res[n_col + 8:, LANES:]
            return carry

        lax.fori_loop(0, 4, pair_step, 0)
        if g == 2:
            gather_second()

    def narrow(c):
        def one(to, carry):
            send[to, c] = wide[pl.ds((to * cols + c) * skip, m_loc), :].astype(BF16)
            return carry

        lax.fori_loop(0, n_src, one, 0, unroll=4)

    def send_batch(c, b):
        for to_aux, to_x in batch(zs, ys, xs, b):
            push(send.at[to_aux * n_x + to_x, c], own.at[c, me], col_send.at[c], col_recv.at[c], aux=to_aux, x=to_x)

    narrow(0)
    for b in range(4):
        for to_aux, to_x in batch(zs, ys, xs, b):
            push(gam, gall.at[me], msg_send.at[0], msg_recv.at[0], aux=to_aux, x=to_x)
    gall[me] = gam[...]
    for b in range(4):
        send_batch(0, b)
    for c in range(1, cols):
        narrow(c)
    for c in range(cols):
        own[c, me] = send[me, c]

    for b in range(4):
        send_batch(1, b)

    await_bytes(gall.at[pl.ds(1, n_src - 1)], msg_recv.at[0])
    for a in range(n_aux):
        gsum[a] = (gall[n_x * a] + gall[n_x * a + 1]) + (gall[n_x * a + 2] + gall[n_x * a + 3])
    push(gsum, gpeer, msg_send.at[1], msg_recv.at[1], core=1 - core).wait()

    def times_met(blocks):
        return lax.dot_general(jnp.concatenate(blocks, axis=1), met_blk[...], NT, precision=PRECISE, preferred_element_type=F32)

    gfit[...] = times_met([gsum[a] + gpeer[a] for a in range(n_aux)])
    for dz in range(4):
        for dy in range(4):
            if dz or dy:
                push(gfit, fall.at[aux], msg_send.at[2], msg_recv.at[2], aux=zs[dz] * 4 + ys[dy])
    fall[aux] = gfit[...]

    fit[...] = jnp.zeros_like(fit)
    kacc[...] = jnp.zeros_like(kacc)
    pad_rows = 64

    def fitted(src, c, side):
        rows = n_x * m_loc
        for n in range(n_fit // tile):
            tot = None
            for s in range(n_aux // 2):
                left = jnp.concatenate([src[c, pl.ds((2 * s + t) * n_x, n_x)].reshape(rows, LANES) for t in range(2)], axis=1)
                right = met[pl.ds(2 * s, 2), :, pl.ds(n * tile, tile)].reshape(2 * LANES, tile)
                part = jnp.dot(left, right, preferred_element_type=F32)
                tot = part if tot is None else tot + part
            for b in range(n_x):
                start = pl.multiple_of((side * n_x + b) * pad_rows, pad_rows)
                fit[pl.ds(start, m_loc), pl.ds(n * tile, tile)] = tot[b * m_loc:(b + 1) * m_loc]

    twelve = met.at[pl.ds(0, 12), upper]
    await_bytes(twelve, met_recv.at[2])
    await_bytes(twelve, met_recv.at[3])

    def col_step(c, carry, pump=False):
        def more(b):
            if pump:
                send_batch(c + 2, b)

        more(0)
        await_bytes(own.at[c, pl.ds(1, n_src - 1)], col_recv.at[c])
        swap = push(own.at[c], other.at[c], pair_send.at[c], pair_recv.at[c], core=1 - core)
        fitted(own, c, core)
        more(1)
        swap.wait()
        fitted(other, c, 1 - core)
        more(2)
        for n in range(n_fit // tile):
            hi, mid, lo = split3(fit[:, pl.ds(n * tile, tile)])
            short = [jnp.concatenate([v[pad_rows * b:pad_rows * b + m_loc] for b in range(2 * n_x)], axis=0) for v in (hi, mid, lo)]
            left = jnp.concatenate([short[0], short[0], short[1], short[0], short[1], short[2]], axis=1)
            right = jnp.concatenate([hi, mid, hi, lo, mid, hi], axis=1)
            kacc[...] += lax.dot_general(left, right, NT, preferred_element_type=F32)
            if n == 1:
                more(3)
        return carry

    lax.fori_loop(0, cols - 2, functools.partial(col_step, pump=True), 0)

    await_bytes(fall.at[pl.ds(1, n_aux - 1)], msg_recv.at[2])
    wts = lax.dot_general(met_blk[...], jnp.concatenate([fall[a] for a in range(n_aux)], axis=1), NT, precision=PRECISE, preferred_element_type=F32)
    for d in range(dens):
        wb[d] = jnp.broadcast_to(wts[:, d:d + 1], (LANES, LANES))
    jm[...] = jnp.zeros_like(jm)

    def coul_group(g, carry):
        def q_step(q, acc):
            rows = [ints[t, q, pl.ds(pl.multiple_of(8 * g, 8), 8), :] for t in range(tiles)]
            return tuple(acc[d * tiles + t] + wb[d, pl.ds(q, 1), :] * rows[t] for d in range(dens) for t in range(tiles))

        acc = lax.fori_loop(0, q_loc, q_step, tuple(jnp.zeros((8, LANES), F32) for _ in range(dens * tiles)), unroll=4)
        for d in range(dens):
            for t in range(tiles):
                jm[d // 2, pl.ds(pl.multiple_of((d % 2) * half_rows + 8 * g, 8), 8), pl.ds(LANES * t, LANES)] = acc[d * tiles + t]
        return carry

    lax.fori_loop(0, groups, coul_group, 0)
    for p in range(dens // 2):
        jt[p] = jm[p].T

    for dz in range(4):
        for dy in range(4):
            if dz or dy:
                to_aux = zs[dz] * 4 + ys[dy]
                push(jt.at[:, pl.ds(pl.multiple_of(to_aux * n_out, 8), n_out), :], jall.at[aux], msg_send.at[3], msg_recv.at[3], aux=to_aux)
    jall[aux] = jt[:, pl.ds(pl.multiple_of(aux * n_out, 8), n_out), :]

    lax.fori_loop(cols - 2, cols, col_step, 0)

    width = n_x * pad_rows
    mine = pl.multiple_of(core * width, width)
    theirs = pl.multiple_of((1 - core) * width, width)
    push(kacc.at[:, pl.ds(theirs, width)], kin, msg_send.at[4], msg_recv.at[4], core=1 - core).wait()
    left_side = lax.broadcasted_iota(jnp.int32, (8, LANES), 1) < pad_rows
    for a in range(n_aux):
        start = a // 2 % 2 * (n_x * m_loc) + a // 4 * m_loc + a % 2 * n_out
        for t in range(width // LANES):
            rows = [kacc[pl.ds(start + 8 * i, 8), pl.ds(pl.multiple_of(mine + t * LANES, LANES), LANES)]
                    + kin[pl.ds(start + 8 * i, 8), pl.ds(t * LANES, LANES)] for i in range(3)]
            turned = [pltpu.roll(v, pad_rows, 1) for v in rows]
            kpk[2 * t, pl.ds(16 * a, 8)] = jnp.where(left_side, rows[0], turned[1])
            kpk[2 * t, pl.ds(16 * a + 8, 8)] = rows[2]
            kpk[2 * t + 1, pl.ds(16 * a, 8)] = jnp.where(left_side, turned[0], rows[1])
            kpk[2 * t + 1, pl.ds(16 * a + 8, 8)] = turned[2]

    def block_for(to_aux, to_x):
        return kpk.at[to_x, pl.ds(pl.multiple_of(to_aux * 16, 16), 16)]

    for b in range(4):
        for to_aux, to_x in batch(zs, ys, xs, b):
            push(block_for(to_aux, to_x), kall.at[me], msg_send.at[5], msg_recv.at[5], aux=to_aux, x=to_x)
    kall[me] = kpk[x, pl.ds(pl.multiple_of(aux * 16, 16), 16)]
    await_bytes(jall.at[pl.ds(1, n_aux - 1)], msg_recv.at[3])
    await_bytes(kall.at[pl.ds(1, n_src - 1)], msg_recv.at[5])
    per = n_src // dens
    for d in range(dens):
        coul = jall[0, d // 2]
        for a in range(1, n_aux):
            coul = coul + jall[a, d // 2]
        coul = pltpu.roll(coul, half_rows, 1) if d % 2 else coul
        exch = kall[per * d]
        for i in range(1, per):
            exch = exch + kall[per * d + i]
        exch = jnp.concatenate([exch[:8], pltpu.roll(exch[:8], pad_rows, 1), exch[8:]], axis=0)
        out_ref[d] = 2.0 * coul - exch

    for c in range(cols):
        await_bytes(own.at[c, pl.ds(1, n_src - 1)], col_send.at[c])
    await_bytes(gall.at[pl.ds(1, n_src - 1)], msg_send.at[0])
    await_bytes(fall.at[pl.ds(1, n_aux - 1)], msg_send.at[2])
    await_bytes(jall.at[pl.ds(1, n_aux - 1)], msg_send.at[3])
    await_bytes(kall.at[pl.ds(1, n_src - 1)], msg_send.at[5])
    for i, n in enumerate((3, 3, 12, 12)):
        await_bytes(met.at[pl.ds(0, n), upper], met_send.at[i])


def fock_build(ints_blk, orbitals, metric_blk, n_aux):
    q_loc, m_loc, n_bas = ints_blk.shape
    dens, _, n_occ = orbitals.shape
    n_col = dens * n_occ
    n_x = n_bas // m_loc // 2
    chips = n_aux * n_x
    cols = n_col // chips
    n_fit = n_aux // 2 * LANES
    n_out = n_bas // n_aux
    tiles = n_bas // LANES
    vmem = pl.BlockSpec(memory_space=pltpu.VMEM)
    dma = pltpu.SemaphoreType.DMA
    return pl.pallas_call(
        fock_kernel,
        out_shape=jax.ShapeDtypeStruct((dens, n_out, LANES), F32),
        in_specs=[pl.BlockSpec(memory_space=pl.ANY), vmem, vmem],
        out_specs=vmem,
        scratch_shapes=[
            pltpu.VMEM((tiles, LANES, m_loc + 8, LANES), F32),
            pltpu.VMEM((n_col * (m_loc + 1), LANES), F32),
            pltpu.VMEM((3, n_col, n_bas), BF16),
            pltpu.VMEM((tiles, 8 * m_loc, LANES), F32),
            pltpu.VMEM((LANES, 2 * n_fit), F32),
            pltpu.VMEM((chips, cols, m_loc, LANES), BF16),
            pltpu.VMEM((cols, chips, m_loc, LANES), BF16),
            pltpu.VMEM((cols, chips, m_loc, LANES), BF16),
            pltpu.VMEM((n_aux, LANES, n_fit), BF16),
            pltpu.VMEM((2 * n_x * 64, n_fit), F32),
            pltpu.VMEM((n_bas, 2 * n_x * 64), F32),
            pltpu.VMEM((n_bas, n_x * 64), F32),
            pltpu.VMEM((n_x, 16 * n_aux, LANES), F32),
            pltpu.VMEM((chips, 16, LANES), F32),
            pltpu.VMEM((8, LANES), F32),
            pltpu.VMEM((chips, 8, LANES), F32),
            pltpu.VMEM((n_aux, 8, LANES), F32),
            pltpu.VMEM((n_aux, 8, LANES), F32),
            pltpu.VMEM((8, LANES), F32),
            pltpu.VMEM((n_aux, 8, LANES), F32),
            pltpu.VMEM((dens, LANES, LANES), F32),
            pltpu.VMEM((dens // 2, LANES, n_bas), F32),
            pltpu.VMEM((dens // 2, n_bas, LANES), F32),
            pltpu.VMEM((n_aux, dens // 2, n_out, LANES), F32),
            dma((m_loc // 8, tiles)), dma((4,)), dma((4,)), dma((cols,)), dma((cols,)), dma((cols,)), dma((cols,)), dma((6,)), dma((6,)),
        ],
        compiler_params=pltpu.CompilerParams(vmem_limit_bytes=62 * 1024 * 1024, collective_id=0, has_side_effects=True),
        name='fock_build',
    )(ints_blk, orbitals, metric_blk)


def solution(mesh):
    n_aux, n_orb = mesh.shape['aux'], mesh.shape['orb']
    mesh4 = jax.sharding.Mesh(mesh.devices.reshape(1, n_aux, n_orb // 2, 2), ('sys', 'aux', 'x', 'core'))

    def local_fock(ints_blk, metric_blk, orbitals):
        m_loc = ints_blk.shape[1]
        out = fock_build(ints_blk, orbitals, metric_blk, n_aux)
        return out[:, :, :m_loc].transpose(0, 2, 1)

    return jax.shard_map(
        local_fock, mesh=mesh4,
        in_specs=(P(('sys', 'aux'), ('x', 'core'), None), P(('sys', 'aux'), None), P('sys', None, None)),
        out_specs=P('sys', ('x', 'core'), 'aux'), check_vma=False)
```

```python
import functools

import jax
import jax.numpy as jnp
from jax import lax
from jax.experimental import pallas as pl
from jax.experimental.pallas import tpu as pltpu
from jax.sharding import PartitionSpec as P

PRECISE = lax.Precision.HIGHEST
F32 = jnp.float32
BF16 = jnp.bfloat16
LANES = 128
NT = (((1,), (1,)), ((), ()))


def split3(x):
    hi = x.astype(BF16)
    rest = x - hi.astype(F32)
    mid = rest.astype(BF16)
    lo = (rest - mid.astype(F32)).astype(BF16)
    return hi, mid, lo


def mesh_pos():
    aux = lax.axis_index('aux')
    return aux // 4, lax.rem(aux, 4), lax.axis_index('x'), lax.axis_index('core')


def near():
    z, y, x, _ = mesh_pos()
    return [[lax.rem(p + d, 4) for d in range(4)] for p in (z, y, x)]


def batch(zs, ys, xs, b):
    for dy in range(4):
        for dx in range(4):
            dz = (b + dy + dx) % 4
            if dz or dy or dx:
                yield zs[dz] * 4 + ys[dy], xs[dx]


def push(src, dst, send_sem, recv_sem, **to):
    copy = pltpu.make_async_remote_copy(src, dst, send_sem, recv_sem, device_id=to, device_id_type=pl.DeviceIdType.MESH)
    copy.start()
    return copy


def await_bytes(like, sem):
    pltpu.make_async_copy(like, like, sem).wait()


def fock_kernel(ints_hbm, orb_ref, met_ref, out_ref,
                ints, wide, terms, orow, drows, met_blk, send, own, other, met, fit, kacc, kin, kpk, kall,
                gam, gall, gsum, gpeer, gfit, fall, wb, jm, jt, jall,
                ints_sem, met_send, met_recv, col_send, col_recv, pair_send, pair_recv, msg_send, msg_recv):
    z, y, x, core = mesh_pos()
    zs, ys, xs = near()
    aux = z * 4 + y
    n_src, cols, m_loc, _ = send.shape
    n_aux, _, n_fit = met.shape
    n_x = n_src // n_aux
    me = aux * n_x + x
    tiles, _, m_pad, _ = ints.shape
    q_loc = ints_hbm.shape[0]
    skip = wide.shape[0] // (n_src * cols)
    n_col = n_src * cols
    groups = m_loc // 8
    tile = 256
    n_out = 24
    half_rows = LANES // 2

    copies = [
        [pltpu.make_async_copy(
            ints_hbm.at[:, pl.ds(8 * g, 8), pl.ds(LANES * t, LANES)],
            ints.at[t, pl.ds(0, q_loc), pl.ds(8 * g, 8), :], ints_sem.at[g, t]) for t in range(tiles)]
        for g in range(groups)]
    for group in copies:
        for copy in group:
            copy.start()
    barrier = pltpu.get_barrier_semaphore()

    for b in range(4):
        for to_aux, to_x in batch(zs, ys, xs, b):
            pl.semaphore_signal(barrier, inc=1, device_id={'aux': to_aux, 'x': to_x}, device_id_type=pl.DeviceIdType.MESH)
    pl.semaphore_signal(barrier, inc=1, device_id={'core': 1 - core}, device_id_type=pl.DeviceIdType.MESH)
    met_blk[...] = jnp.zeros_like(met_blk)
    for b in range(n_aux):
        met_blk[pl.ds(0, q_loc), pl.ds(b * LANES, q_loc)] = met_ref[:, b * q_loc:(b + 1) * q_loc]
    met[aux] = met_blk[:, pl.ds(pl.multiple_of(core * n_fit, n_fit), n_fit)].astype(BF16)
    ints[:, pl.ds(q_loc, LANES - q_loc)] = jnp.zeros((tiles, LANES - q_loc, m_pad, LANES), F32)
    flat = ints.reshape(tiles, LANES * m_pad, LANES)
    dens, n_occ, _ = orb_ref.shape
    drows[...] = jnp.zeros_like(drows)
    for d in range(dens):
        for i, term in enumerate(split3(orb_ref[d])):
            terms[i, pl.ds(d * n_occ, n_occ), :] = term
        orow[d] = orb_ref[d].T
        here = orow[d, pl.ds(pl.multiple_of((x * 2 + core) * m_loc, m_loc), m_loc), :]
        full = jnp.dot(here, orb_ref[d], precision=PRECISE, preferred_element_type=F32)
        for t in range(tiles):
            drows[t, pl.ds(d, m_loc, stride=8), :] = full[:, t * LANES:(t + 1) * LANES]
    gam[...] = jnp.zeros_like(gam)

    upper, lower = pl.ds(0, half_rows), pl.ds(half_rows, half_rows)

    def to_y(d, blk, half, n):
        push(met.at[blk, half], met.at[blk, half], met_send.at[n], met_recv.at[n], aux=z * 4 + ys[d])

    def to_z(d, blk, half, n):
        push(met.at[blk, half], met.at[blk, half], met_send.at[n], met_recv.at[n], aux=zs[d] * 4 + y)

    def gather_first():
        for d in (1, 3, 2):
            to_y(d, aux, upper, 0)
            to_z(d, aux, lower, 1)
        for d in (1, 3, 2):
            to_z(d, aux, upper, 2)
            to_y(d, aux, lower, 3)

    def gather_second():
        three = met.at[pl.ds(0, 3), upper]
        await_bytes(three, met_recv.at[0])
        await_bytes(three, met_recv.at[1])
        for b in range(1, 4):
            for d in (1, 3, 2):
                to_z(d, z * 4 + ys[b], upper, 2)
                to_y(d, zs[b] * 4 + y, lower, 3)

    pl.semaphore_wait(barrier, n_src)
    gather_first()
    for g in range(groups):
        for copy in copies[g]:
            copy.wait()

        def pair_step(j, carry, g=g):
            m = 8 * g + 2 * j
            rows = jnp.concatenate([
                jnp.concatenate([flat[t, pl.ds(m + u, LANES, stride=m_pad), :] for t in range(tiles)], axis=1)
                for u in range(2)], axis=0)
            hi, mid, lo = split3(rows)
            right = jnp.concatenate([hi, mid, hi, lo, mid, hi], axis=1)
            at = pl.ds(pl.multiple_of(16 * (4 * g + j), 16), 16)
            drow = jnp.concatenate([drows[t, at, :] for t in range(tiles)], axis=1)
            both = [jnp.concatenate([terms[i], v], axis=0) for i, v in enumerate(split3(drow))]
            left = jnp.concatenate([both[0], both[0], both[1], both[0], both[1], both[2]], axis=1)
            res = lax.dot_general(left, right, NT, preferred_element_type=F32)
            wide[pl.ds(m, n_col, stride=skip), :] = res[:n_col, :LANES]
            wide[pl.ds(m + 1, n_col, stride=skip), :] = res[:n_col, LANES:]
            gam[...] += res[n_col:n_col + 8, :LANES] + res[n_col + 8:, LANES:]
            return carry

        lax.fori_loop(0, 4, pair_step, 0)
        if g == 2:
            gather_second()

    def narrow(c):
        def one(to, carry):
            send[to, c] = wide[pl.ds((to * cols + c) * skip, m_loc), :].astype(BF16)
            return carry

        lax.fori_loop(0, n_src, one, 0, unroll=4)

    def send_batch(c, b):
        for to_aux, to_x in batch(zs, ys, xs, b):
            push(send.at[to_aux * n_x + to_x, c], own.at[c, me], col_send.at[c], col_recv.at[c], aux=to_aux, x=to_x)

    narrow(0)
    for b in range(4):
        for to_aux, to_x in batch(zs, ys, xs, b):
            push(gam, gall.at[me], msg_send.at[0], msg_recv.at[0], aux=to_aux, x=to_x)
    gall[me] = gam[...]
    for b in range(4):
        send_batch(0, b)
    for c in range(1, cols):
        narrow(c)
    for c in range(cols):
        own[c, me] = send[me, c]

    for b in range(4):
        send_batch(1, b)

    await_bytes(gall.at[pl.ds(1, n_src - 1)], msg_recv.at[0])
    for a in range(n_aux):
        gsum[a] = (gall[n_x * a] + gall[n_x * a + 1]) + (gall[n_x * a + 2] + gall[n_x * a + 3])
    push(gsum, gpeer, msg_send.at[1], msg_recv.at[1], core=1 - core).wait()

    def times_met(blocks):
        return lax.dot_general(jnp.concatenate(blocks, axis=1), met_blk[...], NT, precision=PRECISE, preferred_element_type=F32)

    gfit[...] = times_met([gsum[a] + gpeer[a] for a in range(n_aux)])
    for dz in range(4):
        for dy in range(4):
            if dz or dy:
                push(gfit, fall.at[aux], msg_send.at[2], msg_recv.at[2], aux=zs[dz] * 4 + ys[dy])
    fall[aux] = gfit[...]

    fit[...] = jnp.zeros_like(fit)
    kacc[...] = jnp.zeros_like(kacc)
    pad_rows = 64

    def fitted(src, c, side):
        rows = n_x * m_loc
        for n in range(n_fit // tile):
            tot = None
            for s in range(n_aux // 2):
                left = jnp.concatenate([src[c, pl.ds((2 * s + t) * n_x, n_x)].reshape(rows, LANES) for t in range(2)], axis=1)
                right = met[pl.ds(2 * s, 2), :, pl.ds(n * tile, tile)].reshape(2 * LANES, tile)
                part = jnp.dot(left, right, preferred_element_type=F32)
                tot = part if tot is None else tot + part
            for b in range(n_x):
                start = pl.multiple_of((side * n_x + b) * pad_rows, pad_rows)
                fit[pl.ds(start, m_loc), pl.ds(n * tile, tile)] = tot[b * m_loc:(b + 1) * m_loc]

    twelve = met.at[pl.ds(0, 12), upper]
    await_bytes(twelve, met_recv.at[2])
    await_bytes(twelve, met_recv.at[3])

    def col_step(c, carry, pump=(None,) * 4):
        def more(b):
            if pump[b] is not None:
                send_batch(*pump[b])

        more(0)
        await_bytes(own.at[c, pl.ds(1, n_src - 1)], col_recv.at[c])
        swap = push(own.at[c], other.at[c], pair_send.at[c], pair_recv.at[c], core=1 - core)
        fitted(own, c, core)
        more(1)
        swap.wait()
        fitted(other, c, 1 - core)
        more(2)
        for n in range(n_fit // tile):
            hi, mid, lo = split3(fit[:, pl.ds(n * tile, tile)])
            short = [jnp.concatenate([v[pad_rows * b:pad_rows * b + m_loc] for b in range(2 * n_x)], axis=0) for v in (hi, mid, lo)]
            left = jnp.concatenate([short[0], short[0], short[1], short[0], short[1], short[2]], axis=1)
            right = jnp.concatenate([hi, mid, hi, lo, mid, hi], axis=1)
            kacc[...] += lax.dot_general(left, right, NT, preferred_element_type=F32)
            if n == 1:
                more(3)
        return carry

    col_step(0, 0, [(2, b) for b in range(4)])
    col_step(1, 0, [(3, 0), None, (3, 1), None])

    await_bytes(fall.at[pl.ds(1, n_aux - 1)], msg_recv.at[2])
    wts = lax.dot_general(met_blk[...], jnp.concatenate([fall[a] for a in range(n_aux)], axis=1), NT, precision=PRECISE, preferred_element_type=F32)
    send_batch(3, 2)
    for d in range(dens):
        wb[d] = jnp.broadcast_to(wts[:, d:d + 1], (LANES, LANES))
    jm[...] = jnp.zeros_like(jm)

    def coul_group(g, carry):
        def q_step(q, acc):
            rows = [ints[t, q, pl.ds(pl.multiple_of(8 * g, 8), 8), :] for t in range(tiles)]
            return tuple(acc[d * tiles + t] + wb[d, pl.ds(q, 1), :] * rows[t] for d in range(dens) for t in range(tiles))

        acc = lax.fori_loop(0, q_loc, q_step, tuple(jnp.zeros((8, LANES), F32) for _ in range(dens * tiles)), unroll=4)
        for d in range(dens):
            for t in range(tiles):
                jm[d // 2, pl.ds(pl.multiple_of((d % 2) * half_rows + 8 * g, 8), 8), pl.ds(LANES * t, LANES)] = acc[d * tiles + t]
        return carry

    lax.fori_loop(0, groups // 2, coul_group, 0)
    send_batch(3, 3)
    lax.fori_loop(groups // 2, groups, coul_group, 0)
    send_batch(4, 0)
    for p in range(dens // 2):
        jt[p] = jm[p].T

    for dz in range(4):
        for dy in range(4):
            if dz or dy:
                to_aux = zs[dz] * 4 + ys[dy]
                push(jt.at[:, pl.ds(pl.multiple_of(to_aux * n_out, 8), n_out), :], jall.at[aux], msg_send.at[3], msg_recv.at[3], aux=to_aux)
    jall[aux] = jt[:, pl.ds(pl.multiple_of(aux * n_out, 8), n_out), :]

    col_step(2, 0, [(4, 1), (4, 2), (4, 3), None])
    lax.fori_loop(3, cols, col_step, 0)

    width = n_x * pad_rows
    mine = pl.multiple_of(core * width, width)
    theirs = pl.multiple_of((1 - core) * width, width)
    push(kacc.at[:, pl.ds(theirs, width)], kin, msg_send.at[4], msg_recv.at[4], core=1 - core).wait()
    left_side = lax.broadcasted_iota(jnp.int32, (8, LANES), 1) < pad_rows
    for a in range(n_aux):
        start = a // 2 % 2 * (n_x * m_loc) + a // 4 * m_loc + a % 2 * n_out
        for t in range(width // LANES):
            rows = [kacc[pl.ds(start + 8 * i, 8), pl.ds(pl.multiple_of(mine + t * LANES, LANES), LANES)]
                    + kin[pl.ds(start + 8 * i, 8), pl.ds(t * LANES, LANES)] for i in range(3)]
            turned = [pltpu.roll(v, pad_rows, 1) for v in rows]
            kpk[2 * t, pl.ds(16 * a, 8)] = jnp.where(left_side, rows[0], turned[1])
            kpk[2 * t, pl.ds(16 * a + 8, 8)] = rows[2]
            kpk[2 * t + 1, pl.ds(16 * a, 8)] = jnp.where(left_side, turned[0], rows[1])
            kpk[2 * t + 1, pl.ds(16 * a + 8, 8)] = turned[2]

    def block_for(to_aux, to_x):
        return kpk.at[to_x, pl.ds(pl.multiple_of(to_aux * 16, 16), 16)]

    for b in range(4):
        for to_aux, to_x in batch(zs, ys, xs, b):
            push(block_for(to_aux, to_x), kall.at[me], msg_send.at[5], msg_recv.at[5], aux=to_aux, x=to_x)
    kall[me] = kpk[x, pl.ds(pl.multiple_of(aux * 16, 16), 16)]
    await_bytes(jall.at[pl.ds(1, n_aux - 1)], msg_recv.at[3])
    await_bytes(kall.at[pl.ds(1, n_src - 1)], msg_recv.at[5])
    per = n_src // dens
    for d in range(dens):
        coul = jall[0, d // 2]
        for a in range(1, n_aux):
            coul = coul + jall[a, d // 2]
        coul = pltpu.roll(coul, half_rows, 1) if d % 2 else coul
        exch = kall[per * d]
        for i in range(1, per):
            exch = exch + kall[per * d + i]
        exch = jnp.concatenate([exch[:8], pltpu.roll(exch[:8], pad_rows, 1), exch[8:]], axis=0)
        out_ref[d] = 2.0 * coul - exch

    for c in range(cols):
        await_bytes(own.at[c, pl.ds(1, n_src - 1)], col_send.at[c])
    await_bytes(gall.at[pl.ds(1, n_src - 1)], msg_send.at[0])
    await_bytes(fall.at[pl.ds(1, n_aux - 1)], msg_send.at[2])
    await_bytes(jall.at[pl.ds(1, n_aux - 1)], msg_send.at[3])
    await_bytes(kall.at[pl.ds(1, n_src - 1)], msg_send.at[5])
    for i, n in enumerate((3, 3, 12, 12)):
        await_bytes(met.at[pl.ds(0, n), upper], met_send.at[i])


def fock_build(ints_blk, orb_cols, metric_blk, n_aux):
    q_loc, m_loc, n_bas = ints_blk.shape
    dens, n_occ, _ = orb_cols.shape
    n_col = dens * n_occ
    n_x = n_bas // m_loc // 2
    chips = n_aux * n_x
    cols = n_col // chips
    n_fit = n_aux // 2 * LANES
    n_out = n_bas // n_aux
    tiles = n_bas // LANES
    vmem = pl.BlockSpec(memory_space=pltpu.VMEM)
    dma = pltpu.SemaphoreType.DMA
    return pl.pallas_call(
        fock_kernel,
        out_shape=jax.ShapeDtypeStruct((dens, n_out, LANES), F32),
        in_specs=[pl.BlockSpec(memory_space=pl.ANY), vmem, vmem],
        out_specs=vmem,
        scratch_shapes=[
            pltpu.VMEM((tiles, LANES, m_loc + 8, LANES), F32),
            pltpu.VMEM((n_col * (m_loc + 1), LANES), F32),
            pltpu.VMEM((3, n_col, n_bas), BF16),
            pltpu.VMEM((dens, n_bas, n_occ), F32),
            pltpu.VMEM((tiles, 8 * m_loc, LANES), F32),
            pltpu.VMEM((LANES, 2 * n_fit), F32),
            pltpu.VMEM((chips, cols, m_loc, LANES), BF16),
            pltpu.VMEM((cols, chips, m_loc, LANES), BF16),
            pltpu.VMEM((cols, chips, m_loc, LANES), BF16),
            pltpu.VMEM((n_aux, LANES, n_fit), BF16),
            pltpu.VMEM((2 * n_x * 64, n_fit), F32),
            pltpu.VMEM((n_bas, 2 * n_x * 64), F32),
            pltpu.VMEM((n_bas, n_x * 64), F32),
            pltpu.VMEM((n_x, 16 * n_aux, LANES), F32),
            pltpu.VMEM((chips, 16, LANES), F32),
            pltpu.VMEM((8, LANES), F32),
            pltpu.VMEM((chips, 8, LANES), F32),
            pltpu.VMEM((n_aux, 8, LANES), F32),
            pltpu.VMEM((n_aux, 8, LANES), F32),
            pltpu.VMEM((8, LANES), F32),
            pltpu.VMEM((n_aux, 8, LANES), F32),
            pltpu.VMEM((dens, LANES, LANES), F32),
            pltpu.VMEM((dens // 2, LANES, n_bas), F32),
            pltpu.VMEM((dens // 2, n_bas, LANES), F32),
            pltpu.VMEM((n_aux, dens // 2, n_out, LANES), F32),
            dma((m_loc // 8, tiles)), dma((4,)), dma((4,)), dma((cols,)), dma((cols,)), dma((cols,)), dma((cols,)), dma((6,)), dma((6,)),
        ],
        compiler_params=pltpu.CompilerParams(vmem_limit_bytes=62 * 1024 * 1024, collective_id=0, has_side_effects=True),
        name='fock_build',
    )(ints_blk, orb_cols, metric_blk)


def solution(mesh):
    n_aux, n_orb = mesh.shape['aux'], mesh.shape['orb']
    mesh4 = jax.sharding.Mesh(mesh.devices.reshape(1, n_aux, n_orb // 2, 2), ('sys', 'aux', 'x', 'core'))

    def local_fock(ints_blk, metric_blk, orbitals):
        m_loc = ints_blk.shape[1]
        out = fock_build(ints_blk, orbitals.transpose(0, 2, 1), metric_blk, n_aux)
        return out[:, :, :m_loc].transpose(0, 2, 1)

    return jax.shard_map(
        local_fock, mesh=mesh4,
        in_specs=(P(('sys', 'aux'), ('x', 'core'), None), P(('sys', 'aux'), None), P('sys', None, None)),
        out_specs=P('sys', ('x', 'core'), 'aux'), check_vma=False)
```

```python
import functools

import jax
import jax.numpy as jnp
from jax import lax
from jax.experimental import pallas as pl
from jax.experimental.pallas import tpu as pltpu
from jax.sharding import PartitionSpec as P

PRECISE = lax.Precision.HIGHEST
F32 = jnp.float32
BF16 = jnp.bfloat16
LANES = 128
NT = (((1,), (1,)), ((), ()))


def split3(x):
    hi = x.astype(BF16)
    rest = x - hi.astype(F32)
    mid = rest.astype(BF16)
    lo = (rest - mid.astype(F32)).astype(BF16)
    return hi, mid, lo


def mesh_pos():
    aux = lax.axis_index('aux')
    return aux // 4, lax.rem(aux, 4), lax.axis_index('x'), lax.axis_index('core')


def near():
    z, y, x, _ = mesh_pos()
    return [[lax.rem(p + d, 4) for d in range(4)] for p in (z, y, x)]


def batch(zs, ys, xs, b):
    for dy in range(4):
        for dx in range(4):
            dz = (b + dy + dx) % 4
            if dz or dy or dx:
                yield zs[dz] * 4 + ys[dy], xs[dx]


def push(src, dst, send_sem, recv_sem, **to):
    copy = pltpu.make_async_remote_copy(src, dst, send_sem, recv_sem, device_id=to, device_id_type=pl.DeviceIdType.MESH)
    copy.start()
    return copy


def await_bytes(like, sem):
    pltpu.make_async_copy(like, like, sem).wait()


def fock_kernel(ints_hbm, orb_ref, met_ref, out_ref,
                ints, wide, terms, orow, drows, met_blk, send, own, other, met, fit, kacc, kin, kpk, kall,
                gam, gall, gsum, gpeer, gfit, fall, wb, jm, jt, jall,
                ints_sem, met_send, met_recv, col_send, col_recv, pair_send, pair_recv, msg_send, msg_recv):
    z, y, x, core = mesh_pos()
    zs, ys, xs = near()
    aux = z * 4 + y
    n_src, cols, m_loc, _ = send.shape
    n_aux, _, n_fit = met.shape
    n_x = n_src // n_aux
    me = aux * n_x + x
    tiles, _, m_pad, _ = ints.shape
    q_loc = ints_hbm.shape[0]
    skip = wide.shape[0] // (n_src * cols)
    n_col = n_src * cols
    groups = m_loc // 8
    tile = 256
    n_out = 24
    half_rows = LANES // 2

    copies = [
        [pltpu.make_async_copy(
            ints_hbm.at[:, pl.ds(8 * g, 8), pl.ds(LANES * t, LANES)],
            ints.at[t, pl.ds(0, q_loc), pl.ds(8 * g, 8), :], ints_sem.at[g, t]) for t in range(tiles)]
        for g in range(groups)]
    for group in copies:
        for copy in group:
            copy.start()
    barrier = pltpu.get_barrier_semaphore()

    for b in range(4):
        for to_aux, to_x in batch(zs, ys, xs, b):
            pl.semaphore_signal(barrier, inc=1, device_id={'aux': to_aux, 'x': to_x}, device_id_type=pl.DeviceIdType.MESH)
    pl.semaphore_signal(barrier, inc=1, device_id={'core': 1 - core}, device_id_type=pl.DeviceIdType.MESH)
    met_blk[...] = jnp.zeros_like(met_blk)
    for b in range(n_aux):
        met_blk[pl.ds(0, q_loc), pl.ds(b * LANES, q_loc)] = met_ref[:, b * q_loc:(b + 1) * q_loc]
    met[aux] = met_blk[:, pl.ds(pl.multiple_of(core * n_fit, n_fit), n_fit)].astype(BF16)
    ints[:, pl.ds(q_loc, LANES - q_loc)] = jnp.zeros((tiles, LANES - q_loc, m_pad, LANES), F32)
    flat = ints.reshape(tiles, LANES * m_pad, LANES)
    dens, n_occ, _ = orb_ref.shape
    drows[...] = jnp.zeros_like(drows)
    for d in range(dens):
        for i, term in enumerate(split3(orb_ref[d])):
            terms[i, pl.ds(d * n_occ, n_occ), :] = term
        orow[d] = orb_ref[d].T
        here = orow[d, pl.ds(pl.multiple_of((x * 2 + core) * m_loc, m_loc), m_loc), :]
        full = jnp.dot(here, orb_ref[d], precision=PRECISE, preferred_element_type=F32)
        for t in range(tiles):
            drows[t, pl.ds(d, m_loc, stride=8), :] = full[:, t * LANES:(t + 1) * LANES]
    gam[...] = jnp.zeros_like(gam)

    upper, lower = pl.ds(0, half_rows), pl.ds(half_rows, half_rows)

    def along(axis, blk, start, n_rows, d, sem):
        part = met.at[blk, pl.ds(start, n_rows)]
        push(part, part, met_send.at[sem], met_recv.at[sem], aux=z * 4 + ys[d] if axis else zs[d] * 4 + y)

    def spread(axis, blk, start, sem):
        for d in (1, 3):
            along(axis, blk, start, half_rows, d, sem)

    def pass_on(axis, before, after, start, sem):
        along(axis, before, start, half_rows // 2, 1, sem)
        along(axis, after, start + half_rows // 2, half_rows // 2, 3, sem)

    def at(dz, dy):
        return zs[dz] * 4 + ys[dy]

    blocks_in = (2, 2, 2, 2, 1, 1, 4, 4, 2, 2, 1, 1, 2, 2, 1, 1)

    def got(sem):
        await_bytes(met.at[pl.ds(0, blocks_in[sem]), upper], met_recv.at[sem])

    def gather(stage):
        low = half_rows
        if stage == 0:
            spread(1, aux, 0, 0)
            spread(0, aux, low, 1)
            spread(0, aux, 0, 2)
            spread(1, aux, low, 3)
        if stage == 1:
            got(0)
            got(1)
            pass_on(1, at(0, 3), at(0, 1), 0, 4)
            pass_on(0, at(3, 0), at(1, 0), low, 5)
            for d in (1, 3):
                spread(0, at(0, d), 0, 6)
                spread(1, at(d, 0), low, 7)
        if stage == 2:
            got(4)
            got(5)
            spread(0, at(0, 2), 0, 8)
            spread(1, at(2, 0), low, 9)
            got(2)
            got(3)
            pass_on(0, at(3, 0), at(1, 0), 0, 10)
            pass_on(1, at(0, 3), at(0, 1), low, 11)
        if stage == 3:
            got(6)
            got(7)
            for d in (1, 3):
                pass_on(0, at(3, d), at(1, d), 0, 12)
                pass_on(1, at(d, 3), at(d, 1), low, 13)
        if stage == 4:
            got(8)
            got(9)
            pass_on(0, at(3, 2), at(1, 2), 0, 14)
            pass_on(1, at(2, 3), at(2, 1), low, 15)

    pl.semaphore_wait(barrier, n_src)
    gather(0)
    for g in range(groups):
        for copy in copies[g]:
            copy.wait()

        def pair_step(j, carry, g=g):
            m = 8 * g + 2 * j
            rows = jnp.concatenate([
                jnp.concatenate([flat[t, pl.ds(m + u, LANES, stride=m_pad), :] for t in range(tiles)], axis=1)
                for u in range(2)], axis=0)
            hi, mid, lo = split3(rows)
            right = jnp.concatenate([hi, mid, hi, lo, mid, hi], axis=1)
            at = pl.ds(pl.multiple_of(16 * (4 * g + j), 16), 16)
            drow = jnp.concatenate([drows[t, at, :] for t in range(tiles)], axis=1)
            both = [jnp.concatenate([terms[i], v], axis=0) for i, v in enumerate(split3(drow))]
            left = jnp.concatenate([both[0], both[0], both[1], both[0], both[1], both[2]], axis=1)
            res = lax.dot_general(left, right, NT, preferred_element_type=F32)
            wide[pl.ds(m, n_col, stride=skip), :] = res[:n_col, :LANES]
            wide[pl.ds(m + 1, n_col, stride=skip), :] = res[:n_col, LANES:]
            gam[...] += res[n_col:n_col + 8, :LANES] + res[n_col + 8:, LANES:]
            return carry

        lax.fori_loop(0, 4, pair_step, 0)
        if g in (1, 2, 4, 5):
            gather(g if g < 3 else g - 1)

    def narrow(c):
        def one(to, carry):
            send[to, c] = wide[pl.ds((to * cols + c) * skip, m_loc), :].astype(BF16)
            return carry

        lax.fori_loop(0, n_src, one, 0, unroll=4)

    def send_batch(c, b):
        for to_aux, to_x in batch(zs, ys, xs, b):
            push(send.at[to_aux * n_x + to_x, c], own.at[c, me], col_send.at[c], col_recv.at[c], aux=to_aux, x=to_x)

    narrow(0)
    for b in range(4):
        for to_aux, to_x in batch(zs, ys, xs, b):
            push(gam, gall.at[me], msg_send.at[0], msg_recv.at[0], aux=to_aux, x=to_x)
    gall[me] = gam[...]
    for b in range(4):
        send_batch(0, b)
    for c in range(1, cols):
        narrow(c)
    for c in range(cols):
        own[c, me] = send[me, c]

    await_bytes(gall.at[pl.ds(1, n_src - 1)], msg_recv.at[0])
    for a in range(n_aux):
        gsum[a] = (gall[n_x * a] + gall[n_x * a + 1]) + (gall[n_x * a + 2] + gall[n_x * a + 3])
    swap = push(gsum, gpeer, msg_send.at[1], msg_recv.at[1], core=1 - core)
    send_batch(1, 0)
    swap.wait()

    def times_met(blocks):
        return lax.dot_general(jnp.concatenate(blocks, axis=1), met_blk[...], NT, precision=PRECISE, preferred_element_type=F32)

    gfit[...] = times_met([gsum[a] + gpeer[a] for a in range(n_aux)])
    for dz in range(4):
        for dy in range(4):
            if dz or dy:
                push(gfit, fall.at[aux], msg_send.at[2], msg_recv.at[2], aux=zs[dz] * 4 + ys[dy])
    fall[aux] = gfit[...]
    send_batch(1, 1)

    fit[...] = jnp.zeros_like(fit)
    kacc[...] = jnp.zeros_like(kacc)
    pad_rows = 64

    def fitted(src, c, side):
        rows = n_x * m_loc
        for n in range(n_fit // tile):
            tot = None
            for s in range(n_aux // 2):
                left = jnp.concatenate([src[c, pl.ds((2 * s + t) * n_x, n_x)].reshape(rows, LANES) for t in range(2)], axis=1)
                right = met[pl.ds(2 * s, 2), :, pl.ds(n * tile, tile)].reshape(2 * LANES, tile)
                part = jnp.dot(left, right, preferred_element_type=F32)
                tot = part if tot is None else tot + part
            for b in range(n_x):
                start = pl.multiple_of((side * n_x + b) * pad_rows, pad_rows)
                fit[pl.ds(start, m_loc), pl.ds(n * tile, tile)] = tot[b * m_loc:(b + 1) * m_loc]

    for sem in range(10, 16):
        got(sem)

    def col_step(c, carry, pump=(None,) * 4):
        def more(b):
            if pump[b] is not None:
                send_batch(*pump[b])

        more(0)
        await_bytes(own.at[c, pl.ds(1, n_src - 1)], col_recv.at[c])
        swap = push(own.at[c], other.at[c], pair_send.at[c], pair_recv.at[c], core=1 - core)
        fitted(own, c, core)
        more(1)
        swap.wait()
        fitted(other, c, 1 - core)
        more(2)
        for n in range(n_fit // tile):
            hi, mid, lo = split3(fit[:, pl.ds(n * tile, tile)])
            short = [jnp.concatenate([v[pad_rows * b:pad_rows * b + m_loc] for b in range(2 * n_x)], axis=0) for v in (hi, mid, lo)]
            left = jnp.concatenate([short[0], short[0], short[1], short[0], short[1], short[2]], axis=1)
            right = jnp.concatenate([hi, mid, hi, lo, mid, hi], axis=1)
            kacc[...] += lax.dot_general(left, right, NT, preferred_element_type=F32)
            if n == 1:
                more(3)
        return carry

    col_step(0, 0, [(1, 2), (1, 3), (2, 0), (2, 1)])
    col_step(1, 0, [(2, 2), (2, 3), (3, 0), None])

    await_bytes(fall.at[pl.ds(1, n_aux - 1)], msg_recv.at[2])
    wts = lax.dot_general(met_blk[...], jnp.concatenate([fall[a] for a in range(n_aux)], axis=1), NT, precision=PRECISE, preferred_element_type=F32)
    send_batch(3, 1)
    for d in range(dens):
        wb[d] = jnp.broadcast_to(wts[:, d:d + 1], (LANES, LANES))
    jm[...] = jnp.zeros_like(jm)

    def coul_group(g, carry):
        def q_step(q, acc):
            rows = [ints[t, q, pl.ds(pl.multiple_of(8 * g, 8), 8), :] for t in range(tiles)]
            return tuple(acc[d * tiles + t] + wb[d, pl.ds(q, 1), :] * rows[t] for d in range(dens) for t in range(tiles))

        acc = lax.fori_loop(0, q_loc, q_step, tuple(jnp.zeros((8, LANES), F32) for _ in range(dens * tiles)), unroll=4)
        for d in range(dens):
            for t in range(tiles):
                jm[d // 2, pl.ds(pl.multiple_of((d % 2) * half_rows + 8 * g, 8), 8), pl.ds(LANES * t, LANES)] = acc[d * tiles + t]
        return carry

    lax.fori_loop(0, groups // 2, coul_group, 0)
    send_batch(3, 2)
    lax.fori_loop(groups // 2, groups, coul_group, 0)
    send_batch(3, 3)
    for p in range(dens // 2):
        jt[p] = jm[p].T

    for dz in range(4):
        for dy in range(4):
            if dz or dy:
                to_aux = zs[dz] * 4 + ys[dy]
                push(jt.at[:, pl.ds(pl.multiple_of(to_aux * n_out, 8), n_out), :], jall.at[aux], msg_send.at[3], msg_recv.at[3], aux=to_aux)
    jall[aux] = jt[:, pl.ds(pl.multiple_of(aux * n_out, 8), n_out), :]

    col_step(2, 0, [(4, 0), (4, 1), (4, 2), (4, 3)])
    lax.fori_loop(3, cols, col_step, 0)

    width = n_x * pad_rows
    mine = pl.multiple_of(core * width, width)
    theirs = pl.multiple_of((1 - core) * width, width)
    push(kacc.at[:, pl.ds(theirs, width)], kin, msg_send.at[4], msg_recv.at[4], core=1 - core).wait()
    left_side = lax.broadcasted_iota(jnp.int32, (8, LANES), 1) < pad_rows
    for a in range(n_aux):
        start = a // 2 % 2 * (n_x * m_loc) + a // 4 * m_loc + a % 2 * n_out
        for t in range(width // LANES):
            rows = [kacc[pl.ds(start + 8 * i, 8), pl.ds(pl.multiple_of(mine + t * LANES, LANES), LANES)]
                    + kin[pl.ds(start + 8 * i, 8), pl.ds(t * LANES, LANES)] for i in range(3)]
            turned = [pltpu.roll(v, pad_rows, 1) for v in rows]
            kpk[2 * t, pl.ds(16 * a, 8)] = jnp.where(left_side, rows[0], turned[1])
            kpk[2 * t, pl.ds(16 * a + 8, 8)] = rows[2]
            kpk[2 * t + 1, pl.ds(16 * a, 8)] = jnp.where(left_side, turned[0], rows[1])
            kpk[2 * t + 1, pl.ds(16 * a + 8, 8)] = turned[2]

    def block_for(to_aux, to_x):
        return kpk.at[to_x, pl.ds(pl.multiple_of(to_aux * 16, 16), 16)]

    for b in range(4):
        for to_aux, to_x in batch(zs, ys, xs, b):
            push(block_for(to_aux, to_x), kall.at[me], msg_send.at[5], msg_recv.at[5], aux=to_aux, x=to_x)
    kall[me] = kpk[x, pl.ds(pl.multiple_of(aux * 16, 16), 16)]
    await_bytes(jall.at[pl.ds(1, n_aux - 1)], msg_recv.at[3])
    await_bytes(kall.at[pl.ds(1, n_src - 1)], msg_recv.at[5])
    per = n_src // dens
    for d in range(dens):
        coul = jall[0, d // 2]
        for a in range(1, n_aux):
            coul = coul + jall[a, d // 2]
        coul = pltpu.roll(coul, half_rows, 1) if d % 2 else coul
        exch = kall[per * d]
        for i in range(1, per):
            exch = exch + kall[per * d + i]
        exch = jnp.concatenate([exch[:8], pltpu.roll(exch[:8], pad_rows, 1), exch[8:]], axis=0)
        out_ref[d] = 2.0 * coul - exch

    for c in range(cols):
        await_bytes(own.at[c, pl.ds(1, n_src - 1)], col_send.at[c])
    await_bytes(gall.at[pl.ds(1, n_src - 1)], msg_send.at[0])
    await_bytes(fall.at[pl.ds(1, n_aux - 1)], msg_send.at[2])
    await_bytes(jall.at[pl.ds(1, n_aux - 1)], msg_send.at[3])
    await_bytes(kall.at[pl.ds(1, n_src - 1)], msg_send.at[5])
    for i, n in enumerate(blocks_in):
        await_bytes(met.at[pl.ds(0, n), upper], met_send.at[i])


def fock_build(ints_blk, orb_cols, metric_blk, n_aux):
    q_loc, m_loc, n_bas = ints_blk.shape
    dens, n_occ, _ = orb_cols.shape
    n_col = dens * n_occ
    n_x = n_bas // m_loc // 2
    chips = n_aux * n_x
    cols = n_col // chips
    n_fit = n_aux // 2 * LANES
    n_out = n_bas // n_aux
    tiles = n_bas // LANES
    vmem = pl.BlockSpec(memory_space=pltpu.VMEM)
    dma = pltpu.SemaphoreType.DMA
    return pl.pallas_call(
        fock_kernel,
        out_shape=jax.ShapeDtypeStruct((dens, n_out, LANES), F32),
        in_specs=[pl.BlockSpec(memory_space=pl.ANY), vmem, vmem],
        out_specs=vmem,
        scratch_shapes=[
            pltpu.VMEM((tiles, LANES, m_loc + 8, LANES), F32),
            pltpu.VMEM((n_col * (m_loc + 1), LANES), F32),
            pltpu.VMEM((3, n_col, n_bas), BF16),
            pltpu.VMEM((dens, n_bas, n_occ), F32),
            pltpu.VMEM((tiles, 8 * m_loc, LANES), F32),
            pltpu.VMEM((LANES, 2 * n_fit), F32),
            pltpu.VMEM((chips, cols, m_loc, LANES), BF16),
            pltpu.VMEM((cols, chips, m_loc, LANES), BF16),
            pltpu.VMEM((cols, chips, m_loc, LANES), BF16),
            pltpu.VMEM((n_aux, LANES, n_fit), BF16),
            pltpu.VMEM((2 * n_x * 64, n_fit), F32),
            pltpu.VMEM((n_bas, 2 * n_x * 64), F32),
            pltpu.VMEM((n_bas, n_x * 64), F32),
            pltpu.VMEM((n_x, 16 * n_aux, LANES), F32),
            pltpu.VMEM((chips, 16, LANES), F32),
            pltpu.VMEM((8, LANES), F32),
            pltpu.VMEM((chips, 8, LANES), F32),
            pltpu.VMEM((n_aux, 8, LANES), F32),
            pltpu.VMEM((n_aux, 8, LANES), F32),
            pltpu.VMEM((8, LANES), F32),
            pltpu.VMEM((n_aux, 8, LANES), F32),
            pltpu.VMEM((dens, LANES, LANES), F32),
            pltpu.VMEM((dens // 2, LANES, n_bas), F32),
            pltpu.VMEM((dens // 2, n_bas, LANES), F32),
            pltpu.VMEM((n_aux, dens // 2, n_out, LANES), F32),
            dma((m_loc // 8, tiles)), dma((16,)), dma((16,)), dma((cols,)), dma((cols,)), dma((cols,)), dma((cols,)), dma((6,)), dma((6,)),
        ],
        compiler_params=pltpu.CompilerParams(vmem_limit_bytes=62 * 1024 * 1024, collective_id=0, has_side_effects=True),
        name='fock_build',
    )(ints_blk, orb_cols, metric_blk)


def solution(mesh):
    n_aux, n_orb = mesh.shape['aux'], mesh.shape['orb']
    mesh4 = jax.sharding.Mesh(mesh.devices.reshape(1, n_aux, n_orb // 2, 2), ('sys', 'aux', 'x', 'core'))

    def local_fock(ints_blk, metric_blk, orbitals):
        m_loc = ints_blk.shape[1]
        out = fock_build(ints_blk, orbitals.transpose(0, 2, 1), metric_blk, n_aux)
        return out[:, :, :m_loc].transpose(0, 2, 1)

    return jax.shard_map(
        local_fock, mesh=mesh4,
        in_specs=(P(('sys', 'aux'), ('x', 'core'), None), P(('sys', 'aux'), None), P('sys', None, None)),
        out_specs=P('sys', ('x', 'core'), 'aux'), check_vma=False)
```

```python
import functools

import jax
import jax.numpy as jnp
from jax import lax
from jax.experimental import pallas as pl
from jax.experimental.pallas import tpu as pltpu
from jax.sharding import PartitionSpec as P

PRECISE = lax.Precision.HIGHEST
F32 = jnp.float32
BF16 = jnp.bfloat16
LANES = 128
NT = (((1,), (1,)), ((), ()))


def split3(x):
    hi = x.astype(BF16)
    rest = x - hi.astype(F32)
    mid = rest.astype(BF16)
    lo = (rest - mid.astype(F32)).astype(BF16)
    return hi, mid, lo


def mesh_pos():
    aux = lax.axis_index('aux')
    return aux // 4, lax.rem(aux, 4), lax.axis_index('x'), lax.axis_index('core')


def near():
    z, y, x, _ = mesh_pos()
    return [[lax.rem(p + d, 4) for d in range(4)] for p in (z, y, x)]


def batch(zs, ys, xs, b):
    for dy in range(4):
        for dx in range(4):
            dz = (b + dy + dx) % 4
            if dz or dy or dx:
                yield zs[dz] * 4 + ys[dy], xs[dx]


def push(src, dst, send_sem, recv_sem, **to):
    copy = pltpu.make_async_remote_copy(src, dst, send_sem, recv_sem, device_id=to, device_id_type=pl.DeviceIdType.MESH)
    copy.start()
    return copy


def await_bytes(like, sem):
    pltpu.make_async_copy(like, like, sem).wait()


def fock_kernel(ints_hbm, orb_ref, met_ref, out_ref,
                ints, wide, terms, orow, drows, met_blk, send, own, other, met, fit, kacc, kin, kpk, kall,
                gam, gall, gsum, gpeer, gfit, fall, wb, jm, jt, jall,
                ints_sem, met_send, met_recv, col_send, col_recv, pair_send, pair_recv, msg_send, msg_recv):
    z, y, x, core = mesh_pos()
    zs, ys, xs = near()
    aux = z * 4 + y
    n_src, cols, m_loc, _ = send.shape
    n_aux, _, n_fit = met.shape
    n_x = n_src // n_aux
    me = aux * n_x + x
    tiles, _, m_pad, _ = ints.shape
    q_loc = ints_hbm.shape[0]
    skip = wide.shape[0] // (n_src * cols)
    n_col = n_src * cols
    groups = m_loc // 8
    tile = 256
    n_out = 24
    half_rows = LANES // 2

    copies = [
        [pltpu.make_async_copy(
            ints_hbm.at[:, pl.ds(8 * g, 8), pl.ds(LANES * t, LANES)],
            ints.at[t, pl.ds(0, q_loc), pl.ds(8 * g, 8), :], ints_sem.at[g, t]) for t in range(tiles)]
        for g in range(groups)]
    for group in copies:
        for copy in group:
            copy.start()
    barrier = pltpu.get_barrier_semaphore()

    for b in range(4):
        for to_aux, to_x in batch(zs, ys, xs, b):
            pl.semaphore_signal(barrier, inc=1, device_id={'aux': to_aux, 'x': to_x}, device_id_type=pl.DeviceIdType.MESH)
    pl.semaphore_signal(barrier, inc=1, device_id={'core': 1 - core}, device_id_type=pl.DeviceIdType.MESH)
    met_blk[...] = jnp.zeros_like(met_blk)
    for b in range(n_aux):
        met_blk[pl.ds(0, q_loc), pl.ds(b * LANES, q_loc)] = met_ref[:, b * q_loc:(b + 1) * q_loc]
    met[aux] = met_blk[:, pl.ds(pl.multiple_of(core * n_fit, n_fit), n_fit)].astype(BF16)
    ints[:, pl.ds(q_loc, LANES - q_loc)] = jnp.zeros((tiles, LANES - q_loc, m_pad, LANES), F32)
    flat = ints.reshape(tiles, LANES * m_pad, LANES)
    dens, n_occ, _ = orb_ref.shape
    drows[...] = jnp.zeros_like(drows)
    for d in range(dens):
        for i, term in enumerate(split3(orb_ref[d])):
            terms[i, pl.ds(d * n_occ, n_occ), :] = term
        orow[d] = orb_ref[d].T
        here = orow[d, pl.ds(pl.multiple_of((x * 2 + core) * m_loc, m_loc), m_loc), :]
        full = jnp.dot(here, orb_ref[d], precision=PRECISE, preferred_element_type=F32)
        for t in range(tiles):
            drows[t, pl.ds(d, m_loc, stride=8), :] = full[:, t * LANES:(t + 1) * LANES]
    gam[...] = jnp.zeros_like(gam)

    upper, lower = pl.ds(0, half_rows), pl.ds(half_rows, half_rows)

    def along(axis, blk, start, n_rows, d, sem):
        part = met.at[blk, pl.ds(start, n_rows)]
        push(part, part, met_send.at[sem], met_recv.at[sem], aux=z * 4 + ys[d] if axis else zs[d] * 4 + y)

    def spread(axis, blk, start, sem):
        for d in (1, 3):
            along(axis, blk, start, half_rows, d, sem)

    def pass_on(axis, before, after, start, sem):
        along(axis, before, start, half_rows // 2, 1, sem)
        along(axis, after, start + half_rows // 2, half_rows // 2, 3, sem)

    def at(dz, dy):
        return zs[dz] * 4 + ys[dy]

    blocks_in = (2, 2, 2, 2, 1, 1, 4, 4, 2, 2, 1, 1, 2, 2, 1, 1)

    def got(sem):
        await_bytes(met.at[pl.ds(0, blocks_in[sem]), upper], met_recv.at[sem])

    def gather(stage):
        low = half_rows
        if stage == 0:
            spread(1, aux, 0, 0)
            spread(0, aux, low, 1)
            spread(0, aux, 0, 2)
            spread(1, aux, low, 3)
        if stage == 1:
            got(0)
            got(1)
            pass_on(1, at(0, 3), at(0, 1), 0, 4)
            pass_on(0, at(3, 0), at(1, 0), low, 5)
            for d in (1, 3):
                spread(0, at(0, d), 0, 6)
                spread(1, at(d, 0), low, 7)
        if stage == 2:
            got(4)
            got(5)
            spread(0, at(0, 2), 0, 8)
            spread(1, at(2, 0), low, 9)
            got(2)
            got(3)
            pass_on(0, at(3, 0), at(1, 0), 0, 10)
            pass_on(1, at(0, 3), at(0, 1), low, 11)
        if stage == 3:
            got(6)
            got(7)
            for d in (1, 3):
                pass_on(0, at(3, d), at(1, d), 0, 12)
                pass_on(1, at(d, 3), at(d, 1), low, 13)
        if stage == 4:
            got(8)
            got(9)
            pass_on(0, at(3, 2), at(1, 2), 0, 14)
            pass_on(1, at(2, 3), at(2, 1), low, 15)

    pl.semaphore_wait(barrier, n_src)
    gather(0)
    for g in range(groups):
        for copy in copies[g]:
            copy.wait()

        def pair_step(j, carry, g=g):
            m = 8 * g + 2 * j
            rows = jnp.concatenate([
                jnp.concatenate([flat[t, pl.ds(m + u, LANES, stride=m_pad), :] for t in range(tiles)], axis=1)
                for u in range(2)], axis=0)
            hi, mid, lo = split3(rows)
            right = jnp.concatenate([hi, mid, hi, lo, mid, hi], axis=1)
            at = pl.ds(pl.multiple_of(16 * (4 * g + j), 16), 16)
            drow = jnp.concatenate([drows[t, at, :] for t in range(tiles)], axis=1)
            both = [jnp.concatenate([terms[i], v], axis=0) for i, v in enumerate(split3(drow))]
            left = jnp.concatenate([both[0], both[0], both[1], both[0], both[1], both[2]], axis=1)
            res = lax.dot_general(left, right, NT, preferred_element_type=F32)
            wide[pl.ds(m, n_col, stride=skip), :] = res[:n_col, :LANES]
            wide[pl.ds(m + 1, n_col, stride=skip), :] = res[:n_col, LANES:]
            gam[...] += res[n_col:n_col + 8, :LANES] + res[n_col + 8:, LANES:]
            return carry

        lax.fori_loop(0, 4, pair_step, 0)
        if g in (1, 2, 4, 5):
            gather(g if g < 3 else g - 1)

    def narrow(c):
        def one(to, carry):
            send[to, c] = wide[pl.ds((to * cols + c) * skip, m_loc), :].astype(BF16)
            return carry

        lax.fori_loop(0, n_src, one, 0, unroll=4)

    def send_batch(c, b):
        for to_aux, to_x in batch(zs, ys, xs, b):
            push(send.at[to_aux * n_x + to_x, c], own.at[c, me], col_send.at[c], col_recv.at[c], aux=to_aux, x=to_x)

    narrow(0)
    for b in range(4):
        for to_aux, to_x in batch(zs, ys, xs, b):
            push(gam, gall.at[me], msg_send.at[0], msg_recv.at[0], aux=to_aux, x=to_x)
    gall[me] = gam[...]
    send_batch(0, 0)
    for c in range(1, cols):
        narrow(c)
    send_batch(0, 1)
    for c in range(cols):
        own[c, me] = send[me, c]

    await_bytes(gall.at[pl.ds(1, n_src - 1)], msg_recv.at[0])
    for a in range(n_aux):
        gsum[a] = (gall[n_x * a] + gall[n_x * a + 1]) + (gall[n_x * a + 2] + gall[n_x * a + 3])
    swap = push(gsum, gpeer, msg_send.at[1], msg_recv.at[1], core=1 - core)
    send_batch(0, 2)
    swap.wait()

    def times_met(blocks):
        return lax.dot_general(jnp.concatenate(blocks, axis=1), met_blk[...], NT, precision=PRECISE, preferred_element_type=F32)

    gfit[...] = times_met([gsum[a] + gpeer[a] for a in range(n_aux)])
    for dz in range(4):
        for dy in range(4):
            if dz or dy:
                push(gfit, fall.at[aux], msg_send.at[2], msg_recv.at[2], aux=zs[dz] * 4 + ys[dy])
    fall[aux] = gfit[...]
    send_batch(0, 3)
    send_batch(1, 0)
    send_batch(1, 1)

    fit[...] = jnp.zeros_like(fit)
    kacc[...] = jnp.zeros_like(kacc)
    pad_rows = 64

    def fitted(src, c, side):
        rows = n_x * m_loc
        for n in range(n_fit // tile):
            tot = None
            for s in range(n_aux // 2):
                left = jnp.concatenate([src[c, pl.ds((2 * s + t) * n_x, n_x)].reshape(rows, LANES) for t in range(2)], axis=1)
                right = met[pl.ds(2 * s, 2), :, pl.ds(n * tile, tile)].reshape(2 * LANES, tile)
                part = jnp.dot(left, right, preferred_element_type=F32)
                tot = part if tot is None else tot + part
            for b in range(n_x):
                start = pl.multiple_of((side * n_x + b) * pad_rows, pad_rows)
                fit[pl.ds(start, m_loc), pl.ds(n * tile, tile)] = tot[b * m_loc:(b + 1) * m_loc]

    for sem in range(10, 16):
        got(sem)

    def col_step(c, carry, pump=(None,) * 4):
        def more(b):
            if pump[b] is not None:
                send_batch(*pump[b])

        more(0)
        await_bytes(own.at[c, pl.ds(1, n_src - 1)], col_recv.at[c])
        swap = push(own.at[c], other.at[c], pair_send.at[c], pair_recv.at[c], core=1 - core)
        fitted(own, c, core)
        more(1)
        swap.wait()
        fitted(other, c, 1 - core)
        more(2)
        for n in range(n_fit // tile):
            hi, mid, lo = split3(fit[:, pl.ds(n * tile, tile)])
            short = [jnp.concatenate([v[pad_rows * b:pad_rows * b + m_loc] for b in range(2 * n_x)], axis=0) for v in (hi, mid, lo)]
            left = jnp.concatenate([short[0], short[0], short[1], short[0], short[1], short[2]], axis=1)
            right = jnp.concatenate([hi, mid, hi, lo, mid, hi], axis=1)
            kacc[...] += lax.dot_general(left, right, NT, preferred_element_type=F32)
            if n == 1:
                more(3)
        return carry

    col_step(0, 0, [(1, 2), (1, 3), (2, 0), (2, 1)])
    col_step(1, 0, [(2, 2), (2, 3), (3, 0), None])

    await_bytes(fall.at[pl.ds(1, n_aux - 1)], msg_recv.at[2])
    wts = lax.dot_general(met_blk[...], jnp.concatenate([fall[a] for a in range(n_aux)], axis=1), NT, precision=PRECISE, preferred_element_type=F32)
    send_batch(3, 1)
    for d in range(dens):
        wb[d] = jnp.broadcast_to(wts[:, d:d + 1], (LANES, LANES))
    jm[...] = jnp.zeros_like(jm)

    def coul_group(g, carry):
        def q_step(q, acc):
            rows = [ints[t, q, pl.ds(pl.multiple_of(8 * g, 8), 8), :] for t in range(tiles)]
            return tuple(acc[d * tiles + t] + wb[d, pl.ds(q, 1), :] * rows[t] for d in range(dens) for t in range(tiles))

        acc = lax.fori_loop(0, q_loc, q_step, tuple(jnp.zeros((8, LANES), F32) for _ in range(dens * tiles)), unroll=4)
        for d in range(dens):
            for t in range(tiles):
                jm[d // 2, pl.ds(pl.multiple_of((d % 2) * half_rows + 8 * g, 8), 8), pl.ds(LANES * t, LANES)] = acc[d * tiles + t]
        return carry

    lax.fori_loop(0, groups // 2, coul_group, 0)
    send_batch(3, 2)
    lax.fori_loop(groups // 2, groups, coul_group, 0)
    send_batch(3, 3)
    for p in range(dens // 2):
        jt[p] = jm[p].T

    for dz in range(4):
        for dy in range(4):
            if dz or dy:
                to_aux = zs[dz] * 4 + ys[dy]
                push(jt.at[:, pl.ds(pl.multiple_of(to_aux * n_out, 8), n_out), :], jall.at[aux], msg_send.at[3], msg_recv.at[3], aux=to_aux)
    jall[aux] = jt[:, pl.ds(pl.multiple_of(aux * n_out, 8), n_out), :]

    col_step(2, 0, [(4, 0), (4, 1), (4, 2), (4, 3)])
    lax.fori_loop(3, cols, col_step, 0)

    width = n_x * pad_rows
    mine = pl.multiple_of(core * width, width)
    theirs = pl.multiple_of((1 - core) * width, width)
    push(kacc.at[:, pl.ds(theirs, width)], kin, msg_send.at[4], msg_recv.at[4], core=1 - core).wait()
    left_side = lax.broadcasted_iota(jnp.int32, (8, LANES), 1) < pad_rows
    for a in range(n_aux):
        start = a // 2 % 2 * (n_x * m_loc) + a // 4 * m_loc + a % 2 * n_out
        for t in range(width // LANES):
            rows = [kacc[pl.ds(start + 8 * i, 8), pl.ds(pl.multiple_of(mine + t * LANES, LANES), LANES)]
                    + kin[pl.ds(start + 8 * i, 8), pl.ds(t * LANES, LANES)] for i in range(3)]
            turned = [pltpu.roll(v, pad_rows, 1) for v in rows]
            kpk[2 * t, pl.ds(16 * a, 8)] = jnp.where(left_side, rows[0], turned[1])
            kpk[2 * t, pl.ds(16 * a + 8, 8)] = rows[2]
            kpk[2 * t + 1, pl.ds(16 * a, 8)] = jnp.where(left_side, turned[0], rows[1])
            kpk[2 * t + 1, pl.ds(16 * a + 8, 8)] = turned[2]

    def block_for(to_aux, to_x):
        return kpk.at[to_x, pl.ds(pl.multiple_of(to_aux * 16, 16), 16)]

    for b in range(4):
        for to_aux, to_x in batch(zs, ys, xs, b):
            push(block_for(to_aux, to_x), kall.at[me], msg_send.at[5], msg_recv.at[5], aux=to_aux, x=to_x)
    kall[me] = kpk[x, pl.ds(pl.multiple_of(aux * 16, 16), 16)]
    await_bytes(jall.at[pl.ds(1, n_aux - 1)], msg_recv.at[3])
    await_bytes(kall.at[pl.ds(1, n_src - 1)], msg_recv.at[5])
    per = n_src // dens
    for d in range(dens):
        coul = jall[0, d // 2]
        for a in range(1, n_aux):
            coul = coul + jall[a, d // 2]
        coul = pltpu.roll(coul, half_rows, 1) if d % 2 else coul
        exch = kall[per * d]
        for i in range(1, per):
            exch = exch + kall[per * d + i]
        exch = jnp.concatenate([exch[:8], pltpu.roll(exch[:8], pad_rows, 1), exch[8:]], axis=0)
        out_ref[d] = 2.0 * coul - exch

    for c in range(cols):
        await_bytes(own.at[c, pl.ds(1, n_src - 1)], col_send.at[c])
    await_bytes(gall.at[pl.ds(1, n_src - 1)], msg_send.at[0])
    await_bytes(fall.at[pl.ds(1, n_aux - 1)], msg_send.at[2])
    await_bytes(jall.at[pl.ds(1, n_aux - 1)], msg_send.at[3])
    await_bytes(kall.at[pl.ds(1, n_src - 1)], msg_send.at[5])
    for i, n in enumerate(blocks_in):
        await_bytes(met.at[pl.ds(0, n), upper], met_send.at[i])


def fock_build(ints_blk, orb_cols, metric_blk, n_aux):
    q_loc, m_loc, n_bas = ints_blk.shape
    dens, n_occ, _ = orb_cols.shape
    n_col = dens * n_occ
    n_x = n_bas // m_loc // 2
    chips = n_aux * n_x
    cols = n_col // chips
    n_fit = n_aux // 2 * LANES
    n_out = n_bas // n_aux
    tiles = n_bas // LANES
    vmem = pl.BlockSpec(memory_space=pltpu.VMEM)
    dma = pltpu.SemaphoreType.DMA
    return pl.pallas_call(
        fock_kernel,
        out_shape=jax.ShapeDtypeStruct((dens, n_out, LANES), F32),
        in_specs=[pl.BlockSpec(memory_space=pl.ANY), vmem, vmem],
        out_specs=vmem,
        scratch_shapes=[
            pltpu.VMEM((tiles, LANES, m_loc + 8, LANES), F32),
            pltpu.VMEM((n_col * (m_loc + 1), LANES), F32),
            pltpu.VMEM((3, n_col, n_bas), BF16),
            pltpu.VMEM((dens, n_bas, n_occ), F32),
            pltpu.VMEM((tiles, 8 * m_loc, LANES), F32),
            pltpu.VMEM((LANES, 2 * n_fit), F32),
            pltpu.VMEM((chips, cols, m_loc, LANES), BF16),
            pltpu.VMEM((cols, chips, m_loc, LANES), BF16),
            pltpu.VMEM((cols, chips, m_loc, LANES), BF16),
            pltpu.VMEM((n_aux, LANES, n_fit), BF16),
            pltpu.VMEM((2 * n_x * 64, n_fit), F32),
            pltpu.VMEM((n_bas, 2 * n_x * 64), F32),
            pltpu.VMEM((n_bas, n_x * 64), F32),
            pltpu.VMEM((n_x, 16 * n_aux, LANES), F32),
            pltpu.VMEM((chips, 16, LANES), F32),
            pltpu.VMEM((8, LANES), F32),
            pltpu.VMEM((chips, 8, LANES), F32),
            pltpu.VMEM((n_aux, 8, LANES), F32),
            pltpu.VMEM((n_aux, 8, LANES), F32),
            pltpu.VMEM((8, LANES), F32),
            pltpu.VMEM((n_aux, 8, LANES), F32),
            pltpu.VMEM((dens, LANES, LANES), F32),
            pltpu.VMEM((dens // 2, LANES, n_bas), F32),
            pltpu.VMEM((dens // 2, n_bas, LANES), F32),
            pltpu.VMEM((n_aux, dens // 2, n_out, LANES), F32),
            dma((m_loc // 8, tiles)), dma((16,)), dma((16,)), dma((cols,)), dma((cols,)), dma((cols,)), dma((cols,)), dma((6,)), dma((6,)),
        ],
        compiler_params=pltpu.CompilerParams(vmem_limit_bytes=62 * 1024 * 1024, collective_id=0, has_side_effects=True),
        name='fock_build',
    )(ints_blk, orb_cols, metric_blk)


def solution(mesh):
    n_aux, n_orb = mesh.shape['aux'], mesh.shape['orb']
    mesh4 = jax.sharding.Mesh(mesh.devices.reshape(1, n_aux, n_orb // 2, 2), ('sys', 'aux', 'x', 'core'))

    def local_fock(ints_blk, metric_blk, orbitals):
        m_loc = ints_blk.shape[1]
        out = fock_build(ints_blk, orbitals.transpose(0, 2, 1), metric_blk, n_aux)
        return out[:, :, :m_loc].transpose(0, 2, 1)

    return jax.shard_map(
        local_fock, mesh=mesh4,
        in_specs=(P(('sys', 'aux'), ('x', 'core'), None), P(('sys', 'aux'), None), P('sys', None, None)),
        out_specs=P('sys', ('x', 'core'), 'aux'), check_vma=False)
```
